128 devices in a mesh: row: 8 (over z_lo, y), col: 16 (over z_hi, x, core).
Axes of the slice: x: 4, y: 4, z: 4 (z_hi: 2, z_lo: 2; z = z_hi * 2 + z_lo), core: 2. Of those that a mesh axis runs over, the one named last changes fastest.
Arguments:
- vorticity: float32 [3, 128, 128, 128], P(None, 'row', 'col'), may hold values from -18.1 to 18.1
- scalar: float32 [256, 256, 256], P('row', 'col'), may hold values from -6 to 6
Outputs:
- advected: float32 [256, 256, 256], P('row', 'col')
The draws below stay inside these ranges and needn't reach their ends.
All inputs are finite; a program needn't handle non-finite values. Where the reference program divides by a largest or mean magnitude, that divisor is 1e-20 or more.
Results may differ from the reference program's by a relative error of at most 0.0003.
Values sent between devices are 32-bit elements; how exact they have to be, the bound alone decides.
A program may use at most 64 MiB of HBM per device.

```python
import jax
import jax.numpy as jnp

N = 128
NF = 256


def draw_vorticity(key, part):
    coords = jnp.arange(N, dtype=jnp.float32) / (N - 1.0)
    ramp = 0.5 * (coords[:, None] + coords[None, :])
    spread = jnp.exp(jnp.log(3.0) * ramp)
    noise = jnp.clip(jax.random.normal(key, (3, N, N, N), jnp.float32), -6.0, 6.0)
    return noise * spread[None, :, :, None]


def block_scale(rng, dims, cuts, low, high):
    loudness, own = 1.0, jax.random.fold_in(rng, 6)
    for position, blocks in cuts:
        steps = jnp.exp(jax.random.uniform(jax.random.fold_in(own, position), (blocks,), jnp.float32, low / len(cuts), high / len(cuts)))
        loudness = loudness * jnp.repeat(steps, dims[position] // blocks).reshape([-1 if axis == position else 1 for axis in range(len(dims))])
    return loudness


def bell_draw(own_key, shape, scale, limit, shards=(), kind=jnp.bfloat16):
    values = scale * jax.random.normal(own_key, shape, jnp.float32)
    if shards:
        values = values * block_scale(own_key, shape, shards, -0.22, 0.18)
    return jnp.clip(values, -limit, limit).astype(kind)


def setup_inputs(seed: int = 0) -> dict:
    key_list = jax.random.split(jax.random.key(seed), 3)
    return {
        "vorticity": draw_vorticity(jax.random.fold_in(key_list[2], 71), 0),
        "scalar": bell_draw(key_list[1], (NF, NF, NF), 1.0, 6.0, ((0, 8), (1, 16)), jnp.float32),
    }


COURANT = 0.9
EPSILON = 1e-6


def kernel_weight(distance):
    radius = jnp.abs(distance)
    inner_lobe = -(radius - 1.0) * ((((25.0 * radius - 38.0) * radius - 3.0) * radius + 12.0) * radius + 12.0) / 12.0
    middle_lobe = (radius - 1.0) * (radius - 2.0) * (((25.0 * radius - 114.0) * radius + 153.0) * radius - 48.0) / 24.0
    outer_cube = (radius - 3.0) * (radius - 3.0) * (radius - 3.0)
    outer_lobe = -(radius - 2.0) * outer_cube * (5.0 * radius - 8.0) / 24.0
    return jnp.where(radius < 1.0, inner_lobe, jnp.where(radius < 2.0, middle_lobe, jnp.where(radius < 3.0, outer_lobe, 0.0)))


def induce(vorticity):
    spectrum = jnp.fft.fftn(vorticity, axes=(1, 2, 3))
    indices = jnp.arange(N, dtype=jnp.int32)
    waves = jnp.where(indices < N // 2, indices, indices - N).astype(jnp.float32)
    nyquist = indices == N // 2
    ywaves = waves[:, None, None]
    zwaves = waves[None, :, None]
    xwaves = waves[None, None, :]
    wave_sq = xwaves * xwaves + ywaves * ywaves + zwaves * zwaves
    banned = nyquist[:, None, None] | nyquist[None, :, None] | nyquist[None, None, :]
    keep = (wave_sq > 0.0) & jnp.logical_not(banned)
    factor = jnp.where(keep, 1.0 / jnp.maximum(wave_sq, 1.0), 0.0)
    cross = jnp.stack([ywaves * spectrum[2] - zwaves * spectrum[1],
                       zwaves * spectrum[0] - xwaves * spectrum[2],
                       xwaves * spectrum[1] - ywaves * spectrum[0]])
    velocity_hat = 1j * cross * factor
    return jnp.real(jnp.fft.ifftn(velocity_hat, axes=(1, 2, 3))).astype(jnp.float32)


def refine(coarse, grid_axis):
    lower = 0.75 * coarse + 0.25 * jnp.roll(coarse, 1, grid_axis)
    upper = 0.75 * coarse + 0.25 * jnp.roll(coarse, -1, grid_axis)
    shape = list(coarse.shape)
    shape[grid_axis] = 2 * shape[grid_axis]
    return jnp.stack([lower, upper], axis=grid_axis + 1).reshape(shape)


def remesh(field, displace, grid_axis):
    summed = jnp.zeros(field.shape, jnp.float32)
    for offset in range(-3, 4):
        summed = summed + jnp.roll(field, offset, grid_axis) * kernel_weight(offset - jnp.roll(displace, offset, grid_axis))
    return summed


def reference(vorticity, scalar):
    velocity = induce(vorticity)
    velocity_peak = jnp.max(jnp.abs(velocity))
    courant_scale = COURANT / (velocity_peak + EPSILON)
    result = scalar
    for component, grid_axis in ((0, 2), (1, 0), (2, 1)):
        fine = refine(refine(refine(velocity[component], 2), 0), 1) * courant_scale
        result = remesh(result, fine, grid_axis)
    return result
```

```python
import functools
import math

import jax
import jax.numpy as jnp
import numpy as np
from jax import lax
from jax.experimental import pallas as pl
from jax.experimental.pallas import tpu as pltpu
from jax.sharding import PartitionSpec as P

COURANT = 0.9
EPSILON = 1e-06
MESH = pl.DeviceIdType.MESH
HIGH = lax.Precision.HIGH

N = 128
ROWS, COLS = 8, 16
CHIPS = 64
YB, ZB = 16, 8
FY, FZ = 32, 16
EY, EZ = 38, 24


def turn(exponent):
    angle = 2.0 * math.pi * np.asarray(exponent, np.float64)
    return np.cos(angle), np.sin(angle)


def left_block(re, im):
    return np.block([[re, -im], [im, re]]).astype(np.float32)


def right_block(re, im):
    return np.block([[re, im], [-im, re]]).astype(np.float32)


@functools.cache
def spectral_tables():
    x = np.arange(N)
    k = np.arange(N // 2)
    cos, sin = turn(k[:, None] * x[None, :] / N)
    forward_x = np.concatenate([cos, -sin]).astype(np.float32)
    weight = np.where(k == 0, 1.0, 2.0)[:, None]
    inverse_x = np.concatenate([weight * cos, -weight * sin]).astype(np.float32)
    high = np.arange(64) // 8
    low = np.arange(64) % 8
    grid = (high[:, None] * high[None, :] + low[:, None] * low[None, :]) / 8.0
    forward_left, inverse_left = [], []
    for core in range(2):
        shift = low * (1 - core) / 16.0
        forward_left.append(left_block(*turn(-(grid + shift[:, None]))))
        inverse_left.append(left_block(*turn(grid + shift[None, :])))
    lane = np.arange(N)
    lane_y, lane_z = lane // 8, lane % 8
    lanes = lane_y[:, None] * lane_y[None, :] / 16.0 + lane_z[:, None] * lane_z[None, :] / 8.0
    forward_right = right_block(*turn(-lanes))
    inverse_right = right_block(*turn(lanes))
    twiddle = []
    waves = []
    for core in range(2):
        phase = high[:, None] * lane_y[None, :] + (low + 8 * core)[:, None] * lane_z[None, :]
        twiddle.append(np.stack(turn(-phase / N)))
        ky = high[:, None] + 8 * lane_y[None, :]
        kz = (low + 8 * core)[:, None] + 16 * lane_z[None, :]
        waves.append(np.stack([np.where(q < N // 2, q, q - N) for q in (ky, kz)]))
    return (
        forward_x,
        np.stack(forward_left),
        np.stack(twiddle).astype(np.float32),
        forward_right,
        np.stack(waves).astype(np.float32),
        inverse_right,
        np.stack(inverse_left),
        inverse_x,
    )


@functools.cache
def refine_tables():
    lines = np.zeros((N, 2 * N))
    for fine in range(2 * N):
        coarse = fine // 2
        lines[coarse, fine] += 0.75
        lines[(coarse + (1 if fine % 2 else -1)) % N, fine] += 0.25
    place = {}
    for y in range(YB):
        for z in range(ZB):
            place[y, z] = y * ZB + z
    for i in range(2):
        for z in range(ZB):
            place[i - 2, z] = 128 + i * ZB + z
            place[YB + i, z] = 144 + i * ZB + z
        for y in range(YB):
            place[y, i - 2] = 160 + i * YB + y
            place[y, ZB + i] = 192 + i * YB + y
    for index, (ys, zs) in enumerate(((-2, -2), (-2, ZB), (YB, -2), (YB, ZB))):
        for i in range(2):
            for j in range(2):
                place[ys + j, zs + i] = 224 + 8 * index + 2 * i + j

    def taps(fine):
        coarse = fine // 2
        return ((coarse, 0.75), (coarse + (1 if fine % 2 else -1), 0.25))

    slots = list(range(FZ)) + [16, 17, 18, None, None, -3, -2, -1]
    block = np.zeros((EY * EZ, 256))
    for row in range(EY):
        for slot, fine_z in enumerate(slots):
            if fine_z is None:
                continue
            for y, wy in taps(row - 3):
                for z, wz in taps(fine_z):
                    block[row * EZ + slot, place[y, z]] += wy * wz
    return lines.astype(np.float32), block.astype(np.float32)


def dot(a, b, contract=(1, 0)):
    return lax.dot_general(
        a,
        b,
        (((contract[0],), (contract[1],)), ((), ())),
        precision=HIGH,
        preferred_element_type=jnp.float32,
    )


def spectral_kernel(
    vort,
    scal,
    fwd_x,
    fwd_left,
    twiddle,
    fwd_right,
    waves,
    inv_right,
    inv_left,
    inv_x,
    rim_out,
    ext_out,
    peak_out,
    s_buf,
    r_buf,
    z_buf,
    zo_buf,
    y_buf,
    yo_buf,
    t_buf,
    u_buf,
    pieces,
    peaks,
    peak_row,
    peak_mine,
    peak_other,
    own_sem,
    send_sem,
    recv_sem,
    scal_send,
    scal_recv,
    rim_send,
    rim_recv,
):
    row = lax.axis_index("row")
    col = lax.axis_index("col")
    core = col % 2
    chip = row * 8 + col // 2
    other = 1 - core
    up_row, down_row = (row + 1) % ROWS, (row + ROWS - 1) % ROWS
    up_col, down_col = (col + 1) % COLS, (col + COLS - 1) % COLS

    own = pltpu.make_async_copy(scal, ext_out.at[pl.ds(3, FY), pl.ds(0, FZ), :], own_sem)
    own.start()

    barrier = pltpu.get_barrier_semaphore()

    def greet(i, carry):
        to = (chip + i) % CHIPS
        pl.semaphore_signal(
            barrier, inc=1, device_id=(to // 8, 2 * (to % 8) + other), device_id_type=MESH
        )
        return carry

    lax.fori_loop(0, CHIPS, greet, 0)
    for to_row in (up_row, down_row):
        pl.semaphore_signal(barrier, inc=1, device_id=(to_row, col), device_id_type=MESH)

    for c in range(3):
        s_buf[c] = dot(fwd_x[...], vort[c], (1, 1)).reshape(2, 64, 128)
    pieces[...] = jnp.zeros_like(pieces)
    own.wait()
    pl.semaphore_wait(barrier, CHIPS + 2)

    def exchange(source, target, index):
        def send(i, carry):
            to = (chip + i) % CHIPS
            pltpu.make_async_remote_copy(
                src_ref=source.at[:, :, pl.ds(to, 1), :],
                dst_ref=target.at[:, :, pl.ds(chip, 1), :],
                send_sem=send_sem.at[index],
                recv_sem=recv_sem.at[index],
                device_id=(to // 8, 2 * (to % 8) + other),
                device_id_type=MESH,
            ).start()
            return carry

        lax.fori_loop(0, CHIPS, send, 0)

    def swap(source, target, index):
        pltpu.make_async_remote_copy(
            src_ref=source,
            dst_ref=target,
            send_sem=send_sem.at[index],
            recv_sem=recv_sem.at[index],
            device_id=(row, col + 1 - 2 * core),
            device_id_type=MESH,
        ).start()

    def arrive(target, index):
        pltpu.make_async_copy(target, target, recv_sem.at[index]).wait()

    def left(source, index):
        pltpu.make_async_copy(source, source, send_sem.at[index]).wait()

    exchange(s_buf, r_buf, 0)

    def scal_copy(i, ys, zs, yt, zt, device):
        return pltpu.make_async_remote_copy(
            src_ref=ext_out.at[pl.ds(*ys), pl.ds(*zs), :],
            dst_ref=ext_out.at[pl.ds(*yt), pl.ds(*zt), :],
            send_sem=scal_send.at[i],
            recv_sem=scal_recv.at[i],
            device_id=device,
            device_id_type=MESH,
        )

    y_first, y_last, y_below, y_above, y_all = (3, 3), (32, 3), (0, 3), (35, 3), (3, FY)
    z_first, z_last, z_below, z_above, z_all = (0, 3), (13, 3), (21, 3), (16, 3), (0, FZ)
    scal_copies = [
        scal_copy(0, y_first, z_all, y_above, z_all, (down_row, col)),
        scal_copy(1, y_last, z_all, y_below, z_all, (up_row, col)),
        scal_copy(2, y_all, z_first, y_all, z_above, (row, down_col)),
        scal_copy(3, y_all, z_last, y_all, z_below, (row, up_col)),
        scal_copy(4, y_first, z_first, y_above, z_above, (down_row, down_col)),
        scal_copy(5, y_first, z_last, y_above, z_below, (down_row, up_col)),
        scal_copy(6, y_last, z_first, y_below, z_above, (up_row, down_col)),
        scal_copy(7, y_last, z_last, y_below, z_below, (up_row, up_col)),
    ]
    for copy in scal_copies:
        copy.start()

    arrive(r_buf, 0)
    for c in range(3):
        z_buf[c] = dot(fwd_left[core], r_buf[c].reshape(128, 128))
    swap(z_buf, zo_buf, 1)
    sign = (1 - 2 * core).astype(jnp.float32)
    tw_re = twiddle[core, 0]
    tw_im = twiddle[core, 1]
    ky = waves[core, 0]
    kz = waves[core, 1]
    kx = chip.astype(jnp.float32)
    k_sq = kx * kx + ky * ky + kz * kz
    keep = (k_sq > 0.0) & (ky > -64.0) & (kz > -64.0)
    factor = jnp.where(keep, 1.0 / jnp.maximum(k_sq, 1.0), 0.0) * (1.0 / (N * N * N))
    arrive(zo_buf, 1)
    omega = []
    for c in range(3):
        joined = z_buf[c] + sign * zo_buf[c]
        re, im = joined[:64], joined[64:]
        pair = jnp.concatenate([re * tw_re - im * tw_im, re * tw_im + im * tw_re], axis=1)
        spectrum = dot(pair, fwd_right[...])
        omega.append((spectrum[:, :128], spectrum[:, 128:]))

    def cross(part):
        w0, w1, w2 = omega[0][part], omega[1][part], omega[2][part]
        return (ky * w2 - kz * w1, kz * w0 - kx * w2, kx * w1 - ky * w0)

    cross_re, cross_im = cross(0), cross(1)
    for c in range(3):
        pair = jnp.concatenate([-cross_im[c] * factor, cross_re[c] * factor], axis=1)
        back = dot(pair, inv_right[...])
        re, im = back[:, :128], back[:, 128:]
        y_buf[c, :64] = re * tw_re + im * tw_im
        y_buf[c, 64:] = im * tw_re - re * tw_im
    swap(y_buf, yo_buf, 2)
    arrive(yo_buf, 2)
    for c in range(3):
        joined = y_buf[c] - sign * yo_buf[c]
        t_buf[c] = dot(inv_left[core], joined).reshape(2, 64, 128)
    exchange(t_buf, u_buf, 3)
    arrive(u_buf, 3)
    top = jnp.zeros((8, 128), jnp.float32)
    for c in range(3):
        velocity = dot(u_buf[c].reshape(128, 128), inv_x[...], (0, 0))
        rim_out[c, :128] = velocity
        top = jnp.maximum(top, jnp.max(jnp.abs(velocity).reshape(16, 8, 128), axis=0))
    peak_row[...] = jnp.broadcast_to(jnp.max(top, axis=0, keepdims=True), (8, 128))

    def peak_send(i, carry):
        to = (chip + i) % CHIPS
        pltpu.make_async_remote_copy(
            src_ref=peak_row.at[pl.ds(0, 1), :],
            dst_ref=peaks.at[pl.ds(chip, 1), :],
            send_sem=send_sem.at[4],
            recv_sem=recv_sem.at[4],
            device_id=(to // 8, 2 * (to % 8) + other),
            device_id_type=MESH,
        ).start()
        return carry

    lax.fori_loop(0, CHIPS, peak_send, 0)

    for c in range(3):
        for i in range(2):
            pieces[c, pl.ds(16 * i, 16), :] = rim_out[c, pl.ds(6 + i, 16, 8), :]
            pieces[c, pl.ds(32 + 16 * i, 16), :] = rim_out[c, pl.ds(i, 16, 8), :]
            for index, (y, z) in enumerate(((14, 6), (14, 0), (0, 6), (0, 0))):
                pieces[c, pl.ds(64 + 8 * index + 2 * i, 2), :] = rim_out[
                    c, pl.ds(8 * y + z + i, 2, 8), :
                ]

    def rim_copy(i, source, start, target, count, device):
        return pltpu.make_async_remote_copy(
            src_ref=source.at[:, pl.ds(start, count), :],
            dst_ref=rim_out.at[:, pl.ds(target, count), :],
            send_sem=rim_send.at[i],
            recv_sem=rim_recv.at[i],
            device_id=device,
            device_id_type=MESH,
        )

    rim_copies = [
        rim_copy(0, rim_out, 112, 128, 16, (up_row, col)),
        rim_copy(1, rim_out, 0, 144, 16, (down_row, col)),
        rim_copy(2, pieces, 0, 160, 32, (row, up_col)),
        rim_copy(3, pieces, 32, 192, 32, (row, down_col)),
        rim_copy(4, pieces, 64, 224, 8, (up_row, up_col)),
        rim_copy(5, pieces, 72, 232, 8, (up_row, down_col)),
        rim_copy(6, pieces, 80, 240, 8, (down_row, up_col)),
        rim_copy(7, pieces, 88, 248, 8, (down_row, down_col)),
    ]
    for copy in rim_copies:
        copy.start()
    arrive(peaks, 4)
    peak_mine[...] = jnp.max(peaks[...].reshape(8, 8, 128), axis=0)
    swap(peak_mine, peak_other, 5)
    arrive(peak_other, 5)
    peak_out[...] = jnp.maximum(peak_mine[...], peak_other[...])
    for copy in scal_copies + rim_copies:
        copy.wait_recv()
    left(s_buf, 0)
    left(z_buf, 1)
    left(y_buf, 2)
    left(t_buf, 3)
    left(peaks, 4)
    left(peak_mine, 5)
    for copy in scal_copies + rim_copies:
        copy.wait_send()


def weights(field, moved):
    size = jnp.abs(moved)
    square = moved * moved
    core = square * (7.0 / 48.0 - size * (0.25 - (5.0 / 48.0) * size))
    even = core * size
    odd = core * moved
    near = 2.0 / 3.0 - square * (1.0 / 6.0)
    far = (square - 1.0) * (1.0 / 24.0)
    near_even = square * near + 15.0 * even
    near_odd = moved * near + 5.0 * odd
    far_even = square * far - 6.0 * even
    far_odd = moved * (far + far) - 4.0 * odd
    centre = 1.0 + square * (0.25 * square - 1.25) - 20.0 * even
    return (
        field * (even - odd),
        field * (far_even - far_odd),
        field * (near_even - near_odd),
        field * centre,
        field * (near_even + near_odd),
        field * (far_even + far_odd),
        field * (even + odd),
    )


def sweep_roll(field, moved, axis):
    below3, below2, below1, centre, above1, above2, above3 = weights(field, moved)
    length = field.shape[axis]

    def up(a):
        return pltpu.roll(a, 1, axis)

    def down(a):
        return pltpu.roll(a, length - 1, axis)

    raised = up(above1 + up(above2 + up(above3)))
    lowered = down(below1 + down(below2 + down(below3)))
    return centre + raised + lowered


def remesh_kernel(rim, ext, peak, lines, block, out, moved, swept):
    top = jnp.max(peak[...], axis=1, keepdims=True)
    top = jnp.max(top, axis=0, keepdims=True)
    scale = COURANT / (top + EPSILON)
    for c in range(3):
        wide = dot(rim[c], lines[...]) * scale
        big = wide.astype(jnp.bfloat16)
        small = (wide - big.astype(jnp.float32)).astype(jnp.bfloat16)
        fine = jnp.dot(block[...], big, preferred_element_type=jnp.float32)
        fine = fine + jnp.dot(block[...], small, preferred_element_type=jnp.float32)
        moved[c] = fine.reshape(EY, EZ, 256)

    def along_x(i, carry):
        swept[i] = sweep_roll(ext[i], moved[0, i], 1)
        return carry

    lax.fori_loop(0, EY, along_x, 0)
    for half in range(2):
        lanes = pl.ds(128 * half, 128)

        def along_y(i, held):
            parts = weights(swept[i, :, lanes], moved[1, i, :, lanes])
            held = held + (jnp.zeros((EZ, 128), jnp.float32),)
            held = tuple(a + b for a, b in zip(held, parts))

            @pl.when(i >= 6)
            def _():
                done = sweep_roll(held[0], moved[2, i - 3, :, lanes], 0)
                out[i - 6, :, lanes] = done[:FZ]

            return held[1:]

        lax.fori_loop(0, EY, along_y, (jnp.zeros((EZ, 128), jnp.float32),) * 6)


def shards(vorticity, scalar):
    tables = [jnp.asarray(t) for t in spectral_tables()]
    lines, block = refine_tables()
    vmem = pl.BlockSpec(memory_space=pltpu.VMEM)
    f32 = jnp.float32
    rim, ext, peak = pl.pallas_call(
        spectral_kernel,
        out_shape=(
            jax.ShapeDtypeStruct((3, 256, 128), f32),
            jax.ShapeDtypeStruct((EY, EZ, 256), f32),
            jax.ShapeDtypeStruct((8, 128), f32),
        ),
        in_specs=[vmem, pl.BlockSpec(memory_space=pl.ANY)] + [vmem] * len(tables),
        out_specs=(vmem, vmem, vmem),
        scratch_shapes=[
            pltpu.VMEM((3, 2, 64, 128), f32),
            pltpu.VMEM((3, 2, 64, 128), f32),
            pltpu.VMEM((3, 128, 128), f32),
            pltpu.VMEM((3, 128, 128), f32),
            pltpu.VMEM((3, 128, 128), f32),
            pltpu.VMEM((3, 128, 128), f32),
            pltpu.VMEM((3, 2, 64, 128), f32),
            pltpu.VMEM((3, 2, 64, 128), f32),
            pltpu.VMEM((3, 96, 128), f32),
            pltpu.VMEM((64, 128), f32),
            pltpu.VMEM((8, 128), f32),
            pltpu.VMEM((8, 128), f32),
            pltpu.VMEM((8, 128), f32),
            pltpu.SemaphoreType.DMA,
            pltpu.SemaphoreType.DMA((6,)),
            pltpu.SemaphoreType.DMA((6,)),
            pltpu.SemaphoreType.DMA((8,)),
            pltpu.SemaphoreType.DMA((8,)),
            pltpu.SemaphoreType.DMA((8,)),
            pltpu.SemaphoreType.DMA((8,)),
        ],
        compiler_params=pltpu.CompilerParams(collective_id=0, has_side_effects=True),
        name="spectral",
    )(vorticity.reshape(3, YB * ZB, N), scalar, *tables)
    return pl.pallas_call(
        remesh_kernel,
        out_shape=jax.ShapeDtypeStruct((FY, FZ, 256), f32),
        in_specs=[vmem] * 5,
        out_specs=vmem,
        scratch_shapes=[
            pltpu.VMEM((3, EY, EZ, 256), f32),
            pltpu.VMEM((EY, EZ, 256), f32),
        ],
        name="remesh",
    )(rim, ext, peak, jnp.asarray(lines), jnp.asarray(block, jnp.bfloat16))


def solution(mesh):
    return jax.shard_map(
        shards,
        mesh=mesh,
        in_specs=(P(None, "row", "col", None), P("row", "col", None)),
        out_specs=P("row", "col", None),
        check_vma=False,
    )
```

```python
import functools
import math

import jax
import jax.numpy as jnp
import numpy as np
from jax import lax
from jax.experimental import pallas as pl
from jax.experimental.pallas import tpu as pltpu
from jax.sharding import PartitionSpec as P

COURANT = 0.9
EPSILON = 1e-06
VMEM_LIMIT = 24 << 20
MESH = pl.DeviceIdType.MESH
HIGH = lax.Precision.HIGH

N = 128
ROWS, COLS = 8, 16
CHIPS = 64
YB, ZB = 16, 8
FY, FZ = 32, 16
SLABS = 2
EY, EZ = 38, 24


def turn(exponent):
    angle = 2.0 * math.pi * np.asarray(exponent, np.float64)
    return np.cos(angle), np.sin(angle)


def left_block(re, im):
    return np.block([[re, -im], [im, re]]).astype(np.float32)


def right_block(re, im):
    return np.block([[re, im], [-im, re]]).astype(np.float32)


@functools.cache
def spectral_tables():
    x = np.arange(N)
    k = np.arange(N // 2)
    cos, sin = turn(k[:, None] * x[None, :] / N)
    forward_x = np.concatenate([cos, -sin]).astype(np.float32)
    weight = np.where(k == 0, 1.0, 2.0)[:, None]
    inverse_x = np.concatenate([weight * cos, -weight * sin]).astype(np.float32)
    high = np.arange(64) // 8
    low = np.arange(64) % 8
    grid = (high[:, None] * high[None, :] + low[:, None] * low[None, :]) / 8.0
    forward_left, inverse_left = [], []
    for core in range(2):
        shift = low * (1 - core) / 16.0
        forward_left.append(left_block(*turn(-(grid + shift[:, None]))))
        inverse_left.append(left_block(*turn(grid + shift[None, :])))
    lane = np.arange(N)
    lane_y, lane_z = lane // 8, lane % 8
    lanes = lane_y[:, None] * lane_y[None, :] / 16.0 + lane_z[:, None] * lane_z[None, :] / 8.0
    forward_right = right_block(*turn(-lanes))
    inverse_right = right_block(*turn(lanes))
    twiddle = []
    waves = []
    for core in range(2):
        phase = high[:, None] * lane_y[None, :] + (low + 8 * core)[:, None] * lane_z[None, :]
        twiddle.append(np.stack(turn(-phase / N)))
        ky = high[:, None] + 8 * lane_y[None, :]
        kz = (low + 8 * core)[:, None] + 16 * lane_z[None, :]
        waves.append(np.stack([np.where(q < N // 2, q, q - N) for q in (ky, kz)]))
    return (
        forward_x,
        np.stack(forward_left),
        np.stack(twiddle).astype(np.float32),
        forward_right,
        np.stack(waves).astype(np.float32),
        inverse_right,
        np.stack(inverse_left),
        inverse_x,
    )


@functools.cache
def refine_tables():
    lines = np.zeros((N, 2 * N))
    for fine in range(2 * N):
        coarse = fine // 2
        lines[coarse, fine] += 0.75
        lines[(coarse + (1 if fine % 2 else -1)) % N, fine] += 0.25
    place = {}
    for y in range(YB):
        for z in range(ZB):
            place[y, z] = y * ZB + z
    for i in range(2):
        for z in range(ZB):
            place[i - 2, z] = 128 + i * ZB + z
            place[YB + i, z] = 144 + i * ZB + z
        for y in range(YB):
            place[y, i - 2] = 160 + i * YB + y
            place[y, ZB + i] = 192 + i * YB + y
    for index, (ys, zs) in enumerate(((-2, -2), (-2, ZB), (YB, -2), (YB, ZB))):
        for i in range(2):
            for j in range(2):
                place[ys + j, zs + i] = 224 + 8 * index + 2 * i + j

    def taps(fine):
        coarse = fine // 2
        return ((coarse, 0.75), (coarse + (1 if fine % 2 else -1), 0.25))

    slots = list(range(FZ)) + [16, 17, 18, None, None, -3, -2, -1]
    block = np.zeros((EY * EZ, 256))
    for row in range(EY):
        for slot, fine_z in enumerate(slots):
            if fine_z is None:
                continue
            for y, wy in taps(row - 3):
                for z, wz in taps(fine_z):
                    block[row * EZ + slot, place[y, z]] += wy * wz
    return lines.astype(np.float32), block.astype(np.float32)


def dot(a, b, contract=(1, 0)):
    return lax.dot_general(
        a,
        b,
        (((contract[0],), (contract[1],)), ((), ())),
        precision=HIGH,
        preferred_element_type=jnp.float32,
    )


def spectral_kernel(
    vort,
    scal,
    fwd_x,
    fwd_left,
    twiddle,
    fwd_right,
    waves,
    inv_right,
    inv_left,
    inv_x,
    rim_out,
    ext_out,
    peak_out,
    s_buf,
    r_buf,
    z_buf,
    zo_buf,
    y_buf,
    yo_buf,
    t_buf,
    u_buf,
    pieces,
    peaks,
    peak_row,
    peak_mine,
    peak_other,
    own_sem,
    send_sem,
    recv_sem,
    scal_send,
    scal_recv,
    rim_send,
    rim_recv,
):
    row = lax.axis_index("row")
    col = lax.axis_index("col")
    core = col % 2
    chip = row * 8 + col // 2
    other = 1 - core
    up_row, down_row = (row + 1) % ROWS, (row + ROWS - 1) % ROWS
    up_col, down_col = (col + 1) % COLS, (col + COLS - 1) % COLS

    own = pltpu.make_async_copy(scal, ext_out.at[pl.ds(3, FY), pl.ds(0, FZ), :], own_sem)
    own.start()

    barrier = pltpu.get_barrier_semaphore()

    def greet(i, carry):
        to = (chip + i) % CHIPS
        pl.semaphore_signal(
            barrier, inc=1, device_id=(to // 8, 2 * (to % 8) + other), device_id_type=MESH
        )
        return carry

    lax.fori_loop(0, CHIPS, greet, 0)
    for to_row in (up_row, down_row):
        pl.semaphore_signal(barrier, inc=1, device_id=(to_row, col), device_id_type=MESH)

    for c in range(3):
        s_buf[c] = dot(fwd_x[...], vort[c], (1, 1)).reshape(2, 64, 128)
    pieces[...] = jnp.zeros_like(pieces)
    own.wait()
    pl.semaphore_wait(barrier, CHIPS + 2)

    def exchange(source, target, index):
        def send(i, carry):
            to = (chip + i) % CHIPS
            pltpu.make_async_remote_copy(
                src_ref=source.at[:, :, pl.ds(to, 1), :],
                dst_ref=target.at[:, :, pl.ds(chip, 1), :],
                send_sem=send_sem.at[index],
                recv_sem=recv_sem.at[index],
                device_id=(to // 8, 2 * (to % 8) + other),
                device_id_type=MESH,
            ).start()
            return carry

        lax.fori_loop(0, CHIPS, send, 0)

    def swap(source, target, index):
        pltpu.make_async_remote_copy(
            src_ref=source,
            dst_ref=target,
            send_sem=send_sem.at[index],
            recv_sem=recv_sem.at[index],
            device_id=(row, col + 1 - 2 * core),
            device_id_type=MESH,
        ).start()

    def arrive(target, index):
        pltpu.make_async_copy(target, target, recv_sem.at[index]).wait()

    def left(source, index):
        pltpu.make_async_copy(source, source, send_sem.at[index]).wait()

    exchange(s_buf, r_buf, 0)

    def scal_copy(i, ys, zs, yt, zt, device):
        return pltpu.make_async_remote_copy(
            src_ref=ext_out.at[pl.ds(*ys), pl.ds(*zs), :],
            dst_ref=ext_out.at[pl.ds(*yt), pl.ds(*zt), :],
            send_sem=scal_send.at[i],
            recv_sem=scal_recv.at[i],
            device_id=device,
            device_id_type=MESH,
        )

    y_first, y_last, y_below, y_above, y_all = (3, 3), (32, 3), (0, 3), (35, 3), (3, FY)
    z_first, z_last, z_below, z_above, z_all = (0, 3), (13, 3), (21, 3), (16, 3), (0, FZ)
    scal_copies = [
        scal_copy(0, y_first, z_all, y_above, z_all, (down_row, col)),
        scal_copy(1, y_last, z_all, y_below, z_all, (up_row, col)),
        scal_copy(2, y_all, z_first, y_all, z_above, (row, down_col)),
        scal_copy(3, y_all, z_last, y_all, z_below, (row, up_col)),
        scal_copy(4, y_first, z_first, y_above, z_above, (down_row, down_col)),
        scal_copy(5, y_first, z_last, y_above, z_below, (down_row, up_col)),
        scal_copy(6, y_last, z_first, y_below, z_above, (up_row, down_col)),
        scal_copy(7, y_last, z_last, y_below, z_below, (up_row, up_col)),
    ]
    for copy in scal_copies:
        copy.start()

    arrive(r_buf, 0)
    for c in range(3):
        z_buf[c] = dot(fwd_left[core], r_buf[c].reshape(128, 128))
    swap(z_buf, zo_buf, 1)
    sign = (1 - 2 * core).astype(jnp.float32)
    tw_re = twiddle[core, 0]
    tw_im = twiddle[core, 1]
    ky = waves[core, 0]
    kz = waves[core, 1]
    kx = chip.astype(jnp.float32)
    k_sq = kx * kx + ky * ky + kz * kz
    keep = (k_sq > 0.0) & (ky > -64.0) & (kz > -64.0)
    factor = jnp.where(keep, 1.0 / jnp.maximum(k_sq, 1.0), 0.0) * (1.0 / (N * N * N))
    arrive(zo_buf, 1)
    omega = []
    for c in range(3):
        joined = z_buf[c] + sign * zo_buf[c]
        re, im = joined[:64], joined[64:]
        pair = jnp.concatenate([re * tw_re - im * tw_im, re * tw_im + im * tw_re], axis=1)
        spectrum = dot(pair, fwd_right[...])
        omega.append((spectrum[:, :128], spectrum[:, 128:]))

    def cross(part):
        w0, w1, w2 = omega[0][part], omega[1][part], omega[2][part]
        return (ky * w2 - kz * w1, kz * w0 - kx * w2, kx * w1 - ky * w0)

    cross_re, cross_im = cross(0), cross(1)
    for c in range(3):
        pair = jnp.concatenate([-cross_im[c] * factor, cross_re[c] * factor], axis=1)
        back = dot(pair, inv_right[...])
        re, im = back[:, :128], back[:, 128:]
        y_buf[c, :64] = re * tw_re + im * tw_im
        y_buf[c, 64:] = im * tw_re - re * tw_im
    swap(y_buf, yo_buf, 2)
    arrive(yo_buf, 2)
    for c in range(3):
        joined = y_buf[c] - sign * yo_buf[c]
        t_buf[c] = dot(inv_left[core], joined).reshape(2, 64, 128)
    exchange(t_buf, u_buf, 3)
    arrive(u_buf, 3)
    top = jnp.zeros((8, 128), jnp.float32)
    for c in range(3):
        velocity = dot(u_buf[c].reshape(128, 128), inv_x[...], (0, 0))
        rim_out[c, :128] = velocity
        top = jnp.maximum(top, jnp.max(jnp.abs(velocity).reshape(16, 8, 128), axis=0))
    peak_row[...] = jnp.broadcast_to(jnp.max(top, axis=0, keepdims=True), (8, 128))

    def peak_send(i, carry):
        to = (chip + i) % CHIPS
        pltpu.make_async_remote_copy(
            src_ref=peak_row.at[pl.ds(0, 1), :],
            dst_ref=peaks.at[pl.ds(chip, 1), :],
            send_sem=send_sem.at[4],
            recv_sem=recv_sem.at[4],
            device_id=(to // 8, 2 * (to % 8) + other),
            device_id_type=MESH,
        ).start()
        return carry

    lax.fori_loop(0, CHIPS, peak_send, 0)

    for c in range(3):
        for i in range(2):
            pieces[c, pl.ds(16 * i, 16), :] = rim_out[c, pl.ds(6 + i, 16, 8), :]
            pieces[c, pl.ds(32 + 16 * i, 16), :] = rim_out[c, pl.ds(i, 16, 8), :]
            for index, (y, z) in enumerate(((14, 6), (14, 0), (0, 6), (0, 0))):
                pieces[c, pl.ds(64 + 8 * index + 2 * i, 2), :] = rim_out[
                    c, pl.ds(8 * y + z + i, 2, 8), :
                ]

    def rim_copy(i, source, start, target, count, device):
        return pltpu.make_async_remote_copy(
            src_ref=source.at[:, pl.ds(start, count), :],
            dst_ref=rim_out.at[:, pl.ds(target, count), :],
            send_sem=rim_send.at[i],
            recv_sem=rim_recv.at[i],
            device_id=device,
            device_id_type=MESH,
        )

    rim_copies = [
        rim_copy(0, rim_out, 112, 128, 16, (up_row, col)),
        rim_copy(1, rim_out, 0, 144, 16, (down_row, col)),
        rim_copy(2, pieces, 0, 160, 32, (row, up_col)),
        rim_copy(3, pieces, 32, 192, 32, (row, down_col)),
        rim_copy(4, pieces, 64, 224, 8, (up_row, up_col)),
        rim_copy(5, pieces, 72, 232, 8, (up_row, down_col)),
        rim_copy(6, pieces, 80, 240, 8, (down_row, up_col)),
        rim_copy(7, pieces, 88, 248, 8, (down_row, down_col)),
    ]
    for copy in rim_copies:
        copy.start()
    arrive(peaks, 4)
    peak_mine[...] = jnp.max(peaks[...].reshape(8, 8, 128), axis=0)
    swap(peak_mine, peak_other, 5)
    arrive(peak_other, 5)
    peak_out[...] = jnp.maximum(peak_mine[...], peak_other[...])
    for copy in scal_copies + rim_copies:
        copy.wait_recv()
    left(s_buf, 0)
    left(z_buf, 1)
    left(y_buf, 2)
    left(t_buf, 3)
    left(peaks, 4)
    left(peak_mine, 5)
    for copy in scal_copies + rim_copies:
        copy.wait_send()


def weights(field, moved):
    size = jnp.abs(moved)
    square = moved * moved
    first = field * moved
    second = first * moved
    core = second * (7.0 / 48.0 - size * (0.25 - (5.0 / 48.0) * size))
    even3 = core * size
    odd3 = core * moved
    bend = first * (square * (1.0 / 24.0) - 1.0 / 24.0)
    even2 = bend * moved - 6.0 * even3
    odd2 = (bend + bend) - 4.0 * odd3
    even1 = 0.5 * second - 4.0 * even2 - 9.0 * even3
    odd1 = 0.5 * first - (odd2 + odd2) - 3.0 * odd3
    side = even1 + even2 + even3
    return (
        even3 - odd3,
        even2 - odd2,
        even1 - odd1,
        field - (side + side),
        even1 + odd1,
        even2 + odd2,
        even3 + odd3,
    )


def sweep_roll(field, moved, axis):
    parts = weights(field, moved)
    length = field.shape[axis]
    total = parts[3]
    for offset in (-3, -2, -1, 1, 2, 3):
        total = total + pltpu.roll(parts[3 + offset], offset % length, axis)
    return total


def remesh_kernel(rim, ext, peak, lines, block, out, moved, swept):
    top = jnp.max(peak[...], axis=1, keepdims=True)
    top = jnp.max(top, axis=0, keepdims=True)
    scale = COURANT / (top + EPSILON)
    for c in range(3):
        wide = dot(rim[c], lines[...]) * scale
        big = wide.astype(jnp.bfloat16)
        small = (wide - big.astype(jnp.float32)).astype(jnp.bfloat16)
        fine = jnp.dot(block[...], big, preferred_element_type=jnp.float32)
        fine = fine + jnp.dot(block[...], small, preferred_element_type=jnp.float32)
        moved[c] = fine.reshape(EY, EZ, 256)

    def along_x(i, carry):
        rows = pl.ds(SLABS * i, SLABS)
        field = ext[rows].reshape(SLABS * EZ, 256)
        swept[rows] = sweep_roll(field, moved[0, rows].reshape(SLABS * EZ, 256), 1).reshape(
            SLABS, EZ, 256
        )
        return carry

    lax.fori_loop(0, EY // SLABS, along_x, 0)
    for half in range(2):
        lanes = pl.ds(128 * half, 128)

        def along_y(i, held):
            parts = weights(swept[i, :, lanes], moved[1, i, :, lanes])
            held = held + (jnp.zeros((EZ, 128), jnp.float32),)
            held = tuple(a + b for a, b in zip(held, parts))

            @pl.when(i >= 6)
            def _():
                done = sweep_roll(held[0], moved[2, i - 3, :, lanes], 0)
                out[i - 6, :, lanes] = done[:FZ]

            return held[1:]

        lax.fori_loop(0, EY, along_y, (jnp.zeros((EZ, 128), jnp.float32),) * 6)


def shards(vorticity, scalar):
    tables = [jnp.asarray(t) for t in spectral_tables()]
    lines, block = refine_tables()
    vmem = pl.BlockSpec(memory_space=pltpu.VMEM)
    f32 = jnp.float32
    rim, ext, peak = pl.pallas_call(
        spectral_kernel,
        out_shape=(
            jax.ShapeDtypeStruct((3, 256, 128), f32),
            jax.ShapeDtypeStruct((EY, EZ, 256), f32),
            jax.ShapeDtypeStruct((8, 128), f32),
        ),
        in_specs=[vmem, pl.BlockSpec(memory_space=pltpu.HBM)] + [vmem] * len(tables),
        out_specs=(vmem, vmem, vmem),
        scratch_shapes=[
            pltpu.VMEM((3, 2, 64, 128), f32),
            pltpu.VMEM((3, 2, 64, 128), f32),
            pltpu.VMEM((3, 128, 128), f32),
            pltpu.VMEM((3, 128, 128), f32),
            pltpu.VMEM((3, 128, 128), f32),
            pltpu.VMEM((3, 128, 128), f32),
            pltpu.VMEM((3, 2, 64, 128), f32),
            pltpu.VMEM((3, 2, 64, 128), f32),
            pltpu.VMEM((3, 96, 128), f32),
            pltpu.VMEM((64, 128), f32),
            pltpu.VMEM((8, 128), f32),
            pltpu.VMEM((8, 128), f32),
            pltpu.VMEM((8, 128), f32),
            pltpu.SemaphoreType.DMA,
            pltpu.SemaphoreType.DMA((6,)),
            pltpu.SemaphoreType.DMA((6,)),
            pltpu.SemaphoreType.DMA((8,)),
            pltpu.SemaphoreType.DMA((8,)),
            pltpu.SemaphoreType.DMA((8,)),
            pltpu.SemaphoreType.DMA((8,)),
        ],
        compiler_params=pltpu.CompilerParams(collective_id=0, has_side_effects=True, vmem_limit_bytes=VMEM_LIMIT),
        name="spectral",
    )(vorticity.reshape(3, YB * ZB, N), scalar, *tables)
    return pl.pallas_call(
        remesh_kernel,
        out_shape=jax.ShapeDtypeStruct((FY, FZ, 256), f32),
        in_specs=[vmem] * 5,
        out_specs=vmem,
        scratch_shapes=[
            pltpu.VMEM((3, EY, EZ, 256), f32),
            pltpu.VMEM((EY, EZ, 256), f32),
        ],
        compiler_params=pltpu.CompilerParams(vmem_limit_bytes=VMEM_LIMIT),
        name="remesh",
    )(rim, ext, peak, jnp.asarray(lines), jnp.asarray(block, jnp.bfloat16))


def solution(mesh):
    return jax.shard_map(
        shards,
        mesh=mesh,
        in_specs=(P(None, "row", "col", None), P("row", "col", None)),
        out_specs=P("row", "col", None),
        check_vma=False,
    )
```

```python
import functools
import math

import jax
import jax.numpy as jnp
import numpy as np
from jax import lax
from jax.experimental import pallas as pl
from jax.experimental.pallas import tpu as pltpu
from jax.sharding import PartitionSpec as P

COURANT = 0.9
EPSILON = 1e-06
VMEM_LIMIT = 24 << 20
MESH = pl.DeviceIdType.MESH
HIGH = lax.Precision.HIGH

N = 128
ROWS, COLS = 8, 16
CHIPS = 64
YB, ZB = 16, 8
FY, FZ = 32, 16
SLABS = 2
EY, EZ = 38, 24


def turn(exponent):
    angle = 2.0 * math.pi * np.asarray(exponent, np.float64)
    return np.cos(angle), np.sin(angle)


def left_block(re, im):
    return np.block([[re, -im], [im, re]]).astype(np.float32)


def right_block(re, im):
    return np.block([[re, im], [-im, re]]).astype(np.float32)


@functools.cache
def spectral_tables():
    x = np.arange(N)
    k = np.arange(N // 2)
    cos, sin = turn(k[:, None] * x[None, :] / N)
    forward_x = np.concatenate([cos, -sin]).astype(np.float32)
    weight = np.where(k == 0, 1.0, 2.0)[:, None]
    inverse_x = np.concatenate([weight * cos, -weight * sin]).astype(np.float32)
    high = np.arange(64) // 8
    low = np.arange(64) % 8
    grid = (high[:, None] * high[None, :] + low[:, None] * low[None, :]) / 8.0
    forward_left, inverse_left = [], []
    for core in range(2):
        shift = low * (1 - core) / 16.0
        forward_left.append(left_block(*turn(-(grid + shift[:, None]))))
        inverse_left.append(left_block(*turn(grid + shift[None, :])))
    lane = np.arange(N)
    lane_y, lane_z = lane // 8, lane % 8
    lanes = lane_y[:, None] * lane_y[None, :] / 16.0 + lane_z[:, None] * lane_z[None, :] / 8.0
    forward_right = right_block(*turn(-lanes))
    inverse_right = right_block(*turn(lanes))
    twiddle = []
    waves = []
    for core in range(2):
        phase = high[:, None] * lane_y[None, :] + (low + 8 * core)[:, None] * lane_z[None, :]
        twiddle.append(np.stack(turn(-phase / N)))
        ky = high[:, None] + 8 * lane_y[None, :]
        kz = (low + 8 * core)[:, None] + 16 * lane_z[None, :]
        waves.append(np.stack([np.where(q < N // 2, q, q - N) for q in (ky, kz)]))
    return (
        forward_x,
        np.stack(forward_left),
        np.stack(twiddle).astype(np.float32),
        forward_right,
        np.stack(waves).astype(np.float32),
        inverse_right,
        np.stack(inverse_left),
        inverse_x,
    )


@functools.cache
def refine_tables():
    lines = np.zeros((N, 2 * N))
    for fine in range(2 * N):
        coarse = fine // 2
        lines[coarse, fine] += 0.75
        lines[(coarse + (1 if fine % 2 else -1)) % N, fine] += 0.25
    place = {}
    for y in range(YB):
        for z in range(ZB):
            place[y, z] = y * ZB + z
    for i in range(2):
        for z in range(ZB):
            place[i - 2, z] = 128 + i * ZB + z
            place[YB + i, z] = 144 + i * ZB + z
        for y in range(YB):
            place[y, i - 2] = 160 + i * YB + y
            place[y, ZB + i] = 192 + i * YB + y
    for index, (ys, zs) in enumerate(((-2, -2), (-2, ZB), (YB, -2), (YB, ZB))):
        for i in range(2):
            for j in range(2):
                place[ys + j, zs + i] = 224 + 8 * index + 2 * i + j

    def taps(fine):
        coarse = fine // 2
        return ((coarse, 0.75), (coarse + (1 if fine % 2 else -1), 0.25))

    slots = list(range(FZ)) + [16, 17, 18, None, None, -3, -2, -1]
    block = np.zeros((EY * EZ, 256))
    for row in range(EY):
        for slot, fine_z in enumerate(slots):
            if fine_z is None:
                continue
            for y, wy in taps(row - 3):
                for z, wz in taps(fine_z):
                    block[row * EZ + slot, place[y, z]] += wy * wz
    return lines.astype(np.float32), block.astype(np.float32)


def dot(a, b, contract=(1, 0)):
    return lax.dot_general(
        a,
        b,
        (((contract[0],), (contract[1],)), ((), ())),
        precision=HIGH,
        preferred_element_type=jnp.float32,
    )


FAR_FIRST = sorted(
    ((dx, dy, dz) for dx in range(4) for dy in range(4) for dz in range(4)),
    key=lambda d: -sum(min(step, 4 - step) for step in d),
)


def spectral_kernel(
    vort_hbm,
    scal,
    *refs,
):
    table_hbm, (rim_out, ext_out, peak_out), refs = refs[:8], refs[8:11], refs[11:]
    vort, tables, refs = refs[0], refs[1:9], refs[9:]
    fwd_x, fwd_left, twiddle, fwd_right, waves, inv_right, inv_left, inv_x = tables
    s_buf, r_buf, z_buf, zo_buf, y_buf, yo_buf, t_buf, u_buf, pieces = refs[:9]
    peaks, peak_row, peak_mine, peak_other = refs[9:13]
    load_sem, send_sem, recv_sem, scal_send, scal_recv, rim_send, rim_recv = refs[13:]

    row = lax.axis_index("row")
    col = lax.axis_index("col")
    core = lax.rem(col, 2)
    half = lax.div(col, 2)
    chip = row * 8 + half
    other = 1 - core
    up_row, down_row = lax.rem(row + 1, ROWS), lax.rem(row + ROWS - 1, ROWS)
    up_col, down_col = lax.rem(col + 1, COLS), lax.rem(col + COLS - 1, COLS)

    loads = [pltpu.make_async_copy(vort_hbm, vort, load_sem.at[0])]
    for i in range(8):
        loads.append(pltpu.make_async_copy(table_hbm[i], tables[i], load_sem.at[1 + i]))
    loads.append(
        pltpu.make_async_copy(
            scal, ext_out.at[pl.ds(3, FY), pl.ds(0, FZ), :], load_sem.at[9]
        )
    )
    for load in loads[:2] + loads[9:] + loads[2:9]:
        load.start()

    y0, x0 = lax.rem(row, 4), lax.rem(half, 4)
    z0 = 2 * lax.div(half, 4) + lax.div(row, 4)
    xs = [lax.rem(x0 + d, 4) for d in range(4)]
    ys = [lax.rem(y0 + d, 4) for d in range(4)]
    zs = [lax.rem(z0 + d, 4) for d in range(4)]
    low = [4 * lax.rem(z, 2) for z in zs]
    high = [4 * lax.div(z, 2) for z in zs]
    to_rows = [[low[dz] + ys[dy] for dz in range(4)] for dy in range(4)]
    to_halves = [[high[dz] + xs[dx] for dz in range(4)] for dx in range(4)]
    chips = [(to_rows[dy][dz], to_halves[dx][dz]) for dx, dy, dz in FAR_FIRST]

    barrier = pltpu.get_barrier_semaphore()
    for to_row, to_half in chips:
        pl.semaphore_signal(
            barrier, inc=1, device_id=(to_row, 2 * to_half + other), device_id_type=MESH
        )
    for to_row in (up_row, down_row):
        pl.semaphore_signal(barrier, inc=1, device_id=(to_row, col), device_id_type=MESH)

    loads[0].wait()
    loads[1].wait()
    for c in range(3):
        s_buf[c] = dot(fwd_x[...], vort[c], (1, 1)).reshape(2, 64, 128)
    pieces[...] = jnp.zeros_like(pieces)
    for load in loads[2:]:
        load.wait()
    pl.semaphore_wait(barrier, CHIPS + 2)

    def exchange(source, target, index):
        for to_row, to_half in chips:
            pltpu.make_async_remote_copy(
                src_ref=source.at[:, :, pl.ds(to_row * 8 + to_half, 1), :],
                dst_ref=target.at[:, :, pl.ds(chip, 1), :],
                send_sem=send_sem.at[index],
                recv_sem=recv_sem.at[index],
                device_id=(to_row, 2 * to_half + other),
                device_id_type=MESH,
            ).start()

    def swap(source, target, index):
        pltpu.make_async_remote_copy(
            src_ref=source,
            dst_ref=target,
            send_sem=send_sem.at[index],
            recv_sem=recv_sem.at[index],
            device_id=(row, col + 1 - 2 * core),
            device_id_type=MESH,
        ).start()

    def arrive(target, index):
        pltpu.make_async_copy(target, target, recv_sem.at[index]).wait()

    def left(source, index):
        pltpu.make_async_copy(source, source, send_sem.at[index]).wait()

    exchange(s_buf, r_buf, 0)

    def scal_copy(i, ys, zs, yt, zt, device):
        return pltpu.make_async_remote_copy(
            src_ref=ext_out.at[pl.ds(*ys), pl.ds(*zs), :],
            dst_ref=ext_out.at[pl.ds(*yt), pl.ds(*zt), :],
            send_sem=scal_send.at[i],
            recv_sem=scal_recv.at[i],
            device_id=device,
            device_id_type=MESH,
        )

    y_first, y_last, y_below, y_above, y_all = (3, 3), (32, 3), (0, 3), (35, 3), (3, FY)
    z_first, z_last, z_below, z_above, z_all = (0, 3), (13, 3), (21, 3), (16, 3), (0, FZ)
    scal_copies = [
        scal_copy(0, y_first, z_all, y_above, z_all, (down_row, col)),
        scal_copy(1, y_last, z_all, y_below, z_all, (up_row, col)),
        scal_copy(2, y_all, z_first, y_all, z_above, (row, down_col)),
        scal_copy(3, y_all, z_last, y_all, z_below, (row, up_col)),
        scal_copy(4, y_first, z_first, y_above, z_above, (down_row, down_col)),
        scal_copy(5, y_first, z_last, y_above, z_below, (down_row, up_col)),
        scal_copy(6, y_last, z_first, y_below, z_above, (up_row, down_col)),
        scal_copy(7, y_last, z_last, y_below, z_below, (up_row, up_col)),
    ]
    for copy in scal_copies:
        copy.start()

    arrive(r_buf, 0)
    for c in range(3):
        z_buf[c] = dot(fwd_left[core], r_buf[c].reshape(128, 128))
    swap(z_buf, zo_buf, 1)
    sign = (1 - 2 * core).astype(jnp.float32)
    tw_re = twiddle[core, 0]
    tw_im = twiddle[core, 1]
    ky = waves[core, 0]
    kz = waves[core, 1]
    kx = chip.astype(jnp.float32)
    k_sq = kx * kx + ky * ky + kz * kz
    keep = (k_sq > 0.0) & (ky > -64.0) & (kz > -64.0)
    factor = jnp.where(keep, 1.0 / jnp.maximum(k_sq, 1.0), 0.0) * (1.0 / (N * N * N))
    arrive(zo_buf, 1)
    omega = []
    for c in range(3):
        joined = z_buf[c] + sign * zo_buf[c]
        re, im = joined[:64], joined[64:]
        pair = jnp.concatenate([re * tw_re - im * tw_im, re * tw_im + im * tw_re], axis=1)
        spectrum = dot(pair, fwd_right[...])
        omega.append((spectrum[:, :128], spectrum[:, 128:]))

    def cross(part):
        w0, w1, w2 = omega[0][part], omega[1][part], omega[2][part]
        return (ky * w2 - kz * w1, kz * w0 - kx * w2, kx * w1 - ky * w0)

    cross_re, cross_im = cross(0), cross(1)
    for c in range(3):
        pair = jnp.concatenate([-cross_im[c] * factor, cross_re[c] * factor], axis=1)
        back = dot(pair, inv_right[...])
        re, im = back[:, :128], back[:, 128:]
        y_buf[c, :64] = re * tw_re + im * tw_im
        y_buf[c, 64:] = im * tw_re - re * tw_im
    swap(y_buf, yo_buf, 2)
    arrive(yo_buf, 2)
    for c in range(3):
        joined = y_buf[c] - sign * yo_buf[c]
        t_buf[c] = dot(inv_left[core], joined).reshape(2, 64, 128)
    exchange(t_buf, u_buf, 3)
    arrive(u_buf, 3)
    top = jnp.zeros((8, 128), jnp.float32)
    for c in range(3):
        velocity = dot(u_buf[c].reshape(128, 128), inv_x[...], (0, 0))
        rim_out[c, :128] = velocity
        top = jnp.maximum(top, jnp.max(jnp.abs(velocity).reshape(16, 8, 128), axis=0))
    peak_row[...] = jnp.broadcast_to(jnp.max(top, axis=0, keepdims=True), (8, 128))

    for to_row, to_half in chips:
        pltpu.make_async_remote_copy(
            src_ref=peak_row.at[pl.ds(0, 1), :],
            dst_ref=peaks.at[pl.ds(chip, 1), :],
            send_sem=send_sem.at[4],
            recv_sem=recv_sem.at[4],
            device_id=(to_row, 2 * to_half + other),
            device_id_type=MESH,
        ).start()

    for c in range(3):
        for i in range(2):
            pieces[c, pl.ds(16 * i, 16), :] = rim_out[c, pl.ds(6 + i, 16, 8), :]
            pieces[c, pl.ds(32 + 16 * i, 16), :] = rim_out[c, pl.ds(i, 16, 8), :]
            for index, (y, z) in enumerate(((14, 6), (14, 0), (0, 6), (0, 0))):
                pieces[c, pl.ds(64 + 8 * index + 2 * i, 2), :] = rim_out[
                    c, pl.ds(8 * y + z + i, 2, 8), :
                ]

    def rim_copy(i, source, start, target, count, device):
        return pltpu.make_async_remote_copy(
            src_ref=source.at[:, pl.ds(start, count), :],
            dst_ref=rim_out.at[:, pl.ds(target, count), :],
            send_sem=rim_send.at[i],
            recv_sem=rim_recv.at[i],
            device_id=device,
            device_id_type=MESH,
        )

    rim_copies = [
        rim_copy(0, rim_out, 112, 128, 16, (up_row, col)),
        rim_copy(1, rim_out, 0, 144, 16, (down_row, col)),
        rim_copy(2, pieces, 0, 160, 32, (row, up_col)),
        rim_copy(3, pieces, 32, 192, 32, (row, down_col)),
        rim_copy(4, pieces, 64, 224, 8, (up_row, up_col)),
        rim_copy(5, pieces, 72, 232, 8, (up_row, down_col)),
        rim_copy(6, pieces, 80, 240, 8, (down_row, up_col)),
        rim_copy(7, pieces, 88, 248, 8, (down_row, down_col)),
    ]
    for copy in rim_copies:
        copy.start()
    arrive(peaks, 4)
    peak_mine[...] = jnp.max(peaks[...].reshape(8, 8, 128), axis=0)
    swap(peak_mine, peak_other, 5)
    arrive(peak_other, 5)
    peak_out[...] = jnp.maximum(peak_mine[...], peak_other[...])
    for copy in scal_copies + rim_copies:
        copy.wait_recv()
    left(s_buf, 0)
    left(z_buf, 1)
    left(y_buf, 2)
    left(t_buf, 3)
    left(peaks, 4)
    left(peak_mine, 5)
    for copy in scal_copies + rim_copies:
        copy.wait_send()


def weights(field, moved):
    size = jnp.abs(moved)
    square = moved * moved
    first = field * moved
    second = first * moved
    core = second * (7.0 / 48.0 - size * (0.25 - (5.0 / 48.0) * size))
    even3 = core * size
    odd3 = core * moved
    bend = first * (square * (1.0 / 24.0) - 1.0 / 24.0)
    even2 = bend * moved - 6.0 * even3
    odd2 = (bend + bend) - 4.0 * odd3
    even1 = 0.5 * second - 4.0 * even2 - 9.0 * even3
    odd1 = 0.5 * first - (odd2 + odd2) - 3.0 * odd3
    side = even1 + even2 + even3
    return (
        even3 - odd3,
        even2 - odd2,
        even1 - odd1,
        field - (side + side),
        even1 + odd1,
        even2 + odd2,
        even3 + odd3,
    )


def sweep_roll(field, moved, axis):
    parts = weights(field, moved)
    length = field.shape[axis]
    total = parts[3]
    for offset in (-3, -2, -1, 1, 2, 3):
        total = total + pltpu.roll(parts[3 + offset], offset % length, axis)
    return total


def remesh_kernel(rim, ext, peak, lines, block, out, moved, swept):
    top = jnp.max(peak[...], axis=1, keepdims=True)
    top = jnp.max(top, axis=0, keepdims=True)
    scale = COURANT / (top + EPSILON)
    for c in range(3):
        wide = dot(rim[c], lines[...]) * scale
        big = wide.astype(jnp.bfloat16)
        small = (wide - big.astype(jnp.float32)).astype(jnp.bfloat16)
        fine = jnp.dot(block[...], big, preferred_element_type=jnp.float32)
        fine = fine + jnp.dot(block[...], small, preferred_element_type=jnp.float32)
        moved[c] = fine.reshape(EY, EZ, 256)

    def along_x(i, carry):
        rows = pl.ds(SLABS * i, SLABS)
        field = ext[rows].reshape(SLABS * EZ, 256)
        swept[rows] = sweep_roll(field, moved[0, rows].reshape(SLABS * EZ, 256), 1).reshape(
            SLABS, EZ, 256
        )
        return carry

    lax.fori_loop(0, EY // SLABS, along_x, 0)
    for half in range(2):
        lanes = pl.ds(128 * half, 128)

        def along_y(i, held):
            parts = weights(swept[i, :, lanes], moved[1, i, :, lanes])
            held = held + (jnp.zeros((EZ, 128), jnp.float32),)
            held = tuple(a + b for a, b in zip(held, parts))

            @pl.when(i >= 6)
            def _():
                done = sweep_roll(held[0], moved[2, i - 3, :, lanes], 0)
                out[i - 6, :, lanes] = done[:FZ]

            return held[1:]

        lax.fori_loop(0, EY, along_y, (jnp.zeros((EZ, 128), jnp.float32),) * 6)


def shards(vorticity, scalar):
    tables = [jnp.asarray(t) for t in spectral_tables()]
    lines, block = refine_tables()
    vmem = pl.BlockSpec(memory_space=pltpu.VMEM)
    f32 = jnp.float32
    operands = [vorticity.reshape(3, YB * ZB, N), scalar] + tables
    rim, ext, peak = pl.pallas_call(
        spectral_kernel,
        out_shape=(
            pltpu.VMEM((3, 256, 128), f32),
            pltpu.VMEM((EY, EZ, 256), f32),
            pltpu.VMEM((8, 128), f32),
        ),
        in_specs=[pl.BlockSpec(memory_space=pltpu.HBM)] * len(operands),
        out_specs=(vmem, vmem, vmem),
        scratch_shapes=[
            pltpu.VMEM((3, 128, 128), f32),
            *[pltpu.VMEM(t.shape, f32) for t in tables],
            pltpu.VMEM((3, 2, 64, 128), f32),
            pltpu.VMEM((3, 2, 64, 128), f32),
            pltpu.VMEM((3, 128, 128), f32),
            pltpu.VMEM((3, 128, 128), f32),
            pltpu.VMEM((3, 128, 128), f32),
            pltpu.VMEM((3, 128, 128), f32),
            pltpu.VMEM((3, 2, 64, 128), f32),
            pltpu.VMEM((3, 2, 64, 128), f32),
            pltpu.VMEM((3, 96, 128), f32),
            pltpu.VMEM((64, 128), f32),
            pltpu.VMEM((8, 128), f32),
            pltpu.VMEM((8, 128), f32),
            pltpu.VMEM((8, 128), f32),
            pltpu.SemaphoreType.DMA((10,)),
            pltpu.SemaphoreType.DMA((6,)),
            pltpu.SemaphoreType.DMA((6,)),
            pltpu.SemaphoreType.DMA((8,)),
            pltpu.SemaphoreType.DMA((8,)),
            pltpu.SemaphoreType.DMA((8,)),
            pltpu.SemaphoreType.DMA((8,)),
        ],
        compiler_params=pltpu.CompilerParams(collective_id=0, has_side_effects=True, vmem_limit_bytes=VMEM_LIMIT),
        name="spectral",
    )(*[pltpu.with_memory_space_constraint(a, pltpu.HBM) for a in operands])
    return pl.pallas_call(
        remesh_kernel,
        out_shape=jax.ShapeDtypeStruct((FY, FZ, 256), f32),
        in_specs=[vmem] * 5,
        out_specs=vmem,
        scratch_shapes=[
            pltpu.VMEM((3, EY, EZ, 256), f32),
            pltpu.VMEM((EY, EZ, 256), f32),
        ],
        compiler_params=pltpu.CompilerParams(vmem_limit_bytes=VMEM_LIMIT),
        name="remesh",
    )(rim, ext, peak, jnp.asarray(lines), jnp.asarray(block, jnp.bfloat16))


def solution(mesh):
    return jax.shard_map(
        shards,
        mesh=mesh,
        in_specs=(P(None, "row", "col", None), P("row", "col", None)),
        out_specs=P("row", "col", None),
        check_vma=False,
    )
```

```python
import functools
import math

import jax
import jax.numpy as jnp
import numpy as np
from jax import lax
from jax.experimental import pallas as pl
from jax.experimental.pallas import tpu as pltpu
from jax.sharding import PartitionSpec as P

COURANT = 0.9
EPSILON = 1e-06
VMEM_LIMIT = 24 << 20
MESH = pl.DeviceIdType.MESH
HIGH = lax.Precision.HIGH

N = 128
ROWS, COLS = 8, 16
CHIPS = 64
YB, ZB = 16, 8
FY, FZ = 32, 16
STEP = 19
EY, EZ = 38, 24


def turn(exponent):
    angle = 2.0 * math.pi * np.asarray(exponent, np.float64)
    return np.cos(angle), np.sin(angle)


def left_block(re, im):
    return np.block([[re, -im], [im, re]]).astype(np.float32)


def right_block(re, im):
    return np.block([[re, im], [-im, re]]).astype(np.float32)


@functools.cache
def spectral_tables():
    x = np.arange(N)
    k = np.arange(N // 2)
    cos, sin = turn(k[:, None] * x[None, :] / N)
    forward_x = np.concatenate([cos, -sin]).astype(np.float32)
    weight = np.where(k == 0, 1.0, 2.0)[:, None]
    inverse_x = np.concatenate([weight * cos, -weight * sin]).astype(np.float32)
    high = np.arange(64) // 8
    low = np.arange(64) % 8
    grid = (high[:, None] * high[None, :] + low[:, None] * low[None, :]) / 8.0
    forward_left, inverse_left = [], []
    for core in range(2):
        shift = low * (1 - core) / 16.0
        forward_left.append(left_block(*turn(-(grid + shift[:, None]))))
        inverse_left.append(left_block(*turn(grid + shift[None, :])))
    lane = np.arange(N)
    lane_y, lane_z = lane // 8, lane % 8
    lanes = lane_y[:, None] * lane_y[None, :] / 16.0 + lane_z[:, None] * lane_z[None, :] / 8.0
    forward_right = right_block(*turn(-lanes))
    inverse_right = right_block(*turn(lanes))
    twiddle = []
    waves = []
    for core in range(2):
        phase = high[:, None] * lane_y[None, :] + (low + 8 * core)[:, None] * lane_z[None, :]
        twiddle.append(np.stack(turn(-phase / N)))
        ky = high[:, None] + 8 * lane_y[None, :]
        kz = (low + 8 * core)[:, None] + 16 * lane_z[None, :]
        waves.append(np.stack([np.where(q < N // 2, q, q - N) for q in (ky, kz)]))
    return (
        forward_x,
        np.stack(forward_left),
        np.stack(twiddle).astype(np.float32),
        forward_right,
        np.stack(waves).astype(np.float32),
        inverse_right,
        np.stack(inverse_left),
        inverse_x,
    )


@functools.cache
def refine_tables():
    lines = np.zeros((N, 2 * N))
    for fine in range(2 * N):
        coarse = fine // 2
        lines[coarse, fine] += 0.75
        lines[(coarse + (1 if fine % 2 else -1)) % N, fine] += 0.25
    place = {}
    for y in range(YB):
        for z in range(ZB):
            place[y, z] = y * ZB + z
    for i in range(2):
        for z in range(ZB):
            place[i - 2, z] = 128 + i * ZB + z
            place[YB + i, z] = 144 + i * ZB + z
        for y in range(YB):
            place[y, i - 2] = 160 + i * YB + y
            place[y, ZB + i] = 192 + i * YB + y
    for index, (ys, zs) in enumerate(((-2, -2), (-2, ZB), (YB, -2), (YB, ZB))):
        for i in range(2):
            for j in range(2):
                place[ys + j, zs + i] = 224 + 8 * index + 2 * i + j

    def taps(fine):
        coarse = fine // 2
        return ((coarse, 0.75), (coarse + (1 if fine % 2 else -1), 0.25))

    slots = list(range(FZ)) + [16, 17, 18, None, None, -3, -2, -1]
    block = np.zeros((EY * EZ, 256))
    for row in range(EY):
        for slot, fine_z in enumerate(slots):
            if fine_z is None:
                continue
            for y, wy in taps(row - 3):
                for z, wz in taps(fine_z):
                    block[row * EZ + slot, place[y, z]] += wy * wz
    return lines.astype(np.float32), block.astype(np.float32)


def dot(a, b, contract=(1, 0)):
    return lax.dot_general(
        a,
        b,
        (((contract[0],), (contract[1],)), ((), ())),
        precision=HIGH,
        preferred_element_type=jnp.float32,
    )


FAR_FIRST = sorted(
    ((dx, dy, dz) for dx in range(4) for dy in range(4) for dz in range(4)),
    key=lambda d: -sum(min(step, 4 - step) for step in d),
)


def spectral_kernel(
    vort_hbm,
    scal,
    *refs,
):
    table_hbm, (moved_out, ext_out, peak_out), refs = refs[:10], refs[10:13], refs[13:]
    vort, tables, refs = refs[0], refs[1:11], refs[11:]
    fwd_x, fwd_left, twiddle, fwd_right, waves, inv_right, inv_left, inv_x, lines, block = tables
    s_buf, r_buf, z_buf, zo_buf, y_buf, yo_buf, t_buf, u_buf, rim, pieces, peaks = refs[:11]
    load_sem, send_sem, recv_sem, scal_send, scal_recv, rim_send, rim_recv = refs[11:]

    row = lax.axis_index("row")
    col = lax.axis_index("col")
    core = lax.rem(col, 2)
    half = lax.div(col, 2)
    chip = row * 8 + half
    other = 1 - core
    up_row, down_row = lax.rem(row + 1, ROWS), lax.rem(row + ROWS - 1, ROWS)
    up_col, down_col = lax.rem(col + 1, COLS), lax.rem(col + COLS - 1, COLS)

    loads = [pltpu.make_async_copy(vort_hbm, vort, load_sem.at[0])]
    for i in range(10):
        loads.append(pltpu.make_async_copy(table_hbm[i], tables[i], load_sem.at[1 + i]))
    loads.append(
        pltpu.make_async_copy(
            scal, ext_out.at[pl.ds(3, FY), pl.ds(0, FZ), :], load_sem.at[11]
        )
    )
    for load in loads[:2] + loads[11:] + loads[2:11]:
        load.start()

    y0, x0 = lax.rem(row, 4), lax.rem(half, 4)
    z0 = 2 * lax.div(half, 4) + lax.div(row, 4)
    xs = [lax.rem(x0 + d, 4) for d in range(4)]
    ys = [lax.rem(y0 + d, 4) for d in range(4)]
    zs = [lax.rem(z0 + d, 4) for d in range(4)]
    low = [4 * lax.rem(z, 2) for z in zs]
    high = [4 * lax.div(z, 2) for z in zs]
    to_rows = [[low[dz] + ys[dy] for dz in range(4)] for dy in range(4)]
    to_halves = [[high[dz] + xs[dx] for dz in range(4)] for dx in range(4)]
    chips = [(to_rows[dy][dz], to_halves[dx][dz]) for dx, dy, dz in FAR_FIRST]

    barrier = pltpu.get_barrier_semaphore()
    for to_row, to_half in chips:
        pl.semaphore_signal(
            barrier, inc=1, device_id=(to_row, 2 * to_half + other), device_id_type=MESH
        )
    for to_row, to_half in chips[:-1]:
        pl.semaphore_signal(
            barrier, inc=1, device_id=(to_row, 2 * to_half + core), device_id_type=MESH
        )

    loads[0].wait()
    loads[1].wait()
    for c in range(3):
        s_buf[c] = dot(fwd_x[...], vort[c], (1, 1)).reshape(2, 64, 128)
    pieces[...] = jnp.zeros_like(pieces)
    for load in loads[2:]:
        load.wait()
    pl.semaphore_wait(barrier, 2 * CHIPS - 1)

    def exchange(source, target, index):
        for to_row, to_half in chips:
            pltpu.make_async_remote_copy(
                src_ref=source.at[:, :, pl.ds(to_row * 8 + to_half, 1), :],
                dst_ref=target.at[:, :, pl.ds(chip, 1), :],
                send_sem=send_sem.at[index],
                recv_sem=recv_sem.at[index],
                device_id=(to_row, 2 * to_half + other),
                device_id_type=MESH,
            ).start()

    def swap(source, target, index):
        pltpu.make_async_remote_copy(
            src_ref=source,
            dst_ref=target,
            send_sem=send_sem.at[index],
            recv_sem=recv_sem.at[index],
            device_id=(row, col + 1 - 2 * core),
            device_id_type=MESH,
        ).start()

    def arrive(target, index):
        pltpu.make_async_copy(target, target, recv_sem.at[index]).wait()

    def left(source, index):
        pltpu.make_async_copy(source, source, send_sem.at[index]).wait()

    exchange(s_buf, r_buf, 0)

    def scal_copy(i, ys, zs, yt, zt, device):
        return pltpu.make_async_remote_copy(
            src_ref=ext_out.at[pl.ds(*ys), pl.ds(*zs), :],
            dst_ref=ext_out.at[pl.ds(*yt), pl.ds(*zt), :],
            send_sem=scal_send.at[i],
            recv_sem=scal_recv.at[i],
            device_id=device,
            device_id_type=MESH,
        )

    y_first, y_last, y_below, y_above, y_all = (3, 3), (32, 3), (0, 3), (35, 3), (3, FY)
    z_first, z_last, z_below, z_above, z_all = (0, 3), (13, 3), (21, 3), (16, 3), (0, FZ)
    scal_copies = [
        scal_copy(0, y_first, z_all, y_above, z_all, (down_row, col)),
        scal_copy(1, y_last, z_all, y_below, z_all, (up_row, col)),
        scal_copy(2, y_all, z_first, y_all, z_above, (row, down_col)),
        scal_copy(3, y_all, z_last, y_all, z_below, (row, up_col)),
        scal_copy(4, y_first, z_first, y_above, z_above, (down_row, down_col)),
        scal_copy(5, y_first, z_last, y_above, z_below, (down_row, up_col)),
        scal_copy(6, y_last, z_first, y_below, z_above, (up_row, down_col)),
        scal_copy(7, y_last, z_last, y_below, z_below, (up_row, up_col)),
    ]
    for copy in scal_copies:
        copy.start()

    arrive(r_buf, 0)
    for c in range(3):
        z_buf[c] = dot(fwd_left[core], r_buf[c].reshape(128, 128))
    swap(z_buf, zo_buf, 1)
    sign = (1 - 2 * core).astype(jnp.float32)
    tw_re = twiddle[core, 0]
    tw_im = twiddle[core, 1]
    ky = waves[core, 0]
    kz = waves[core, 1]
    kx = chip.astype(jnp.float32)
    k_sq = kx * kx + ky * ky + kz * kz
    keep = (k_sq > 0.0) & (ky > -64.0) & (kz > -64.0)
    factor = jnp.where(keep, 1.0 / jnp.maximum(k_sq, 1.0), 0.0) * (1.0 / (N * N * N))
    arrive(zo_buf, 1)
    omega = []
    for c in range(3):
        joined = z_buf[c] + sign * zo_buf[c]
        re, im = joined[:64], joined[64:]
        pair = jnp.concatenate([re * tw_re - im * tw_im, re * tw_im + im * tw_re], axis=1)
        spectrum = dot(pair, fwd_right[...])
        omega.append((spectrum[:, :128], spectrum[:, 128:]))

    def cross(part):
        w0, w1, w2 = omega[0][part], omega[1][part], omega[2][part]
        return (ky * w2 - kz * w1, kz * w0 - kx * w2, kx * w1 - ky * w0)

    cross_re, cross_im = cross(0), cross(1)
    for c in range(3):
        pair = jnp.concatenate([-cross_im[c] * factor, cross_re[c] * factor], axis=1)
        back = dot(pair, inv_right[...])
        re, im = back[:, :128], back[:, 128:]
        y_buf[c, :64] = re * tw_re + im * tw_im
        y_buf[c, 64:] = im * tw_re - re * tw_im
    swap(y_buf, yo_buf, 2)
    arrive(yo_buf, 2)
    for c in range(3):
        joined = y_buf[c] - sign * yo_buf[c]
        t_buf[c] = dot(inv_left[core], joined).reshape(2, 64, 128)
    exchange(t_buf, u_buf, 3)
    arrive(u_buf, 3)
    top = jnp.zeros((8, 128), jnp.float32)
    for c in range(3):
        velocity = dot(u_buf[c].reshape(128, 128), inv_x[...], (0, 0))
        rim[c, :128] = velocity
        top = jnp.maximum(top, jnp.max(jnp.abs(velocity).reshape(16, 8, 128), axis=0))
    mine = row * COLS + col
    peaks[pl.ds(mine, 1), :] = jnp.max(top, axis=0, keepdims=True)
    for to_core, targets in ((other, chips), (core, chips[:-1])):
        for to_row, to_half in targets:
            pltpu.make_async_remote_copy(
                src_ref=peaks.at[pl.ds(mine, 1), :],
                dst_ref=peaks.at[pl.ds(mine, 1), :],
                send_sem=send_sem.at[4],
                recv_sem=recv_sem.at[4],
                device_id=(to_row, 2 * to_half + to_core),
                device_id_type=MESH,
            ).start()

    for c in range(3):
        for i in range(2):
            pieces[c, pl.ds(16 * i, 16), :] = rim[c, pl.ds(6 + i, 16, 8), :]
            pieces[c, pl.ds(32 + 16 * i, 16), :] = rim[c, pl.ds(i, 16, 8), :]
            for index, (y, z) in enumerate(((14, 6), (14, 0), (0, 6), (0, 0))):
                pieces[c, pl.ds(64 + 8 * index + 2 * i, 2), :] = rim[
                    c, pl.ds(8 * y + z + i, 2, 8), :
                ]

    def rim_copy(i, source, start, target, count, device):
        return pltpu.make_async_remote_copy(
            src_ref=source.at[:, pl.ds(start, count), :],
            dst_ref=rim.at[:, pl.ds(target, count), :],
            send_sem=rim_send.at[i],
            recv_sem=rim_recv.at[i],
            device_id=device,
            device_id_type=MESH,
        )

    rim_copies = [
        rim_copy(0, rim, 112, 128, 16, (up_row, col)),
        rim_copy(1, rim, 0, 144, 16, (down_row, col)),
        rim_copy(2, pieces, 0, 160, 32, (row, up_col)),
        rim_copy(3, pieces, 32, 192, 32, (row, down_col)),
        rim_copy(4, pieces, 64, 224, 8, (up_row, up_col)),
        rim_copy(5, pieces, 72, 232, 8, (up_row, down_col)),
        rim_copy(6, pieces, 80, 240, 8, (down_row, up_col)),
        rim_copy(7, pieces, 88, 248, 8, (down_row, down_col)),
    ]
    for copy in rim_copies:
        copy.start()
    for copy in rim_copies:
        copy.wait_recv()
    for c in range(3):
        wide = dot(rim[c], lines[...])
        big = wide.astype(jnp.bfloat16)
        small = (wide - big.astype(jnp.float32)).astype(jnp.bfloat16)
        fine = jnp.dot(block[...], big, preferred_element_type=jnp.float32)
        fine = fine + jnp.dot(block[...], small, preferred_element_type=jnp.float32)
        moved_out[c] = fine.reshape(EY, EZ, 256)
    others = peaks.at[pl.ds(0, 2 * CHIPS - 1), :]
    arrive(others, 4)
    peak_out[...] = jnp.max(peaks[...].reshape(16, 8, 128), axis=0)
    for copy in scal_copies:
        copy.wait_recv()
    left(s_buf, 0)
    left(z_buf, 1)
    left(y_buf, 2)
    left(t_buf, 3)
    left(others, 4)
    for copy in scal_copies + rim_copies:
        copy.wait_send()


def weights(field, moved):
    size = jnp.abs(moved)
    square = moved * moved
    first = field * moved
    second = first * moved
    core = second * (7.0 / 48.0 - size * (0.25 - (5.0 / 48.0) * size))
    even3 = core * size
    odd3 = core * moved
    bend = first * (square * (1.0 / 24.0) - 1.0 / 24.0)
    even2 = bend * moved - 6.0 * even3
    odd2 = (bend + bend) - 4.0 * odd3
    even1 = 0.5 * second - 4.0 * even2 - 9.0 * even3
    odd1 = 0.5 * first - (odd2 + odd2) - 3.0 * odd3
    side = even1 + even2 + even3
    return (
        even3 - odd3,
        even2 - odd2,
        even1 - odd1,
        field - (side + side),
        even1 + odd1,
        even2 + odd2,
        even3 + odd3,
    )


def sweep_roll(field, moved, axis):
    parts = weights(field, moved)
    length = field.shape[axis]
    total = parts[3]
    for offset in (-3, -2, -1, 1, 2, 3):
        total = total + pltpu.roll(parts[3 + offset], offset % length, axis)
    return total


def remesh_kernel(moved, ext, peak, out, swept, landed, shifts):
    top = jnp.max(peak[...], axis=1, keepdims=True)
    top = jnp.max(top, axis=0, keepdims=True)
    scale = COURANT / (top + EPSILON)

    def along_x(i, carry):
        for tile in range(STEP):
            rows = pl.ds(pl.multiple_of(8 * (STEP * i + tile), 8), 8)
            total = sweep_roll(ext[rows], scale * moved[0, rows], 1)
            swept[0, rows] = total[:, :128]
            swept[1, rows] = total[:, 128:]
        return carry

    lax.fori_loop(0, EY * EZ // 8 // STEP, along_x, 0)
    for half in range(2):
        lanes = pl.ds(128 * half, 128)

        def along_y(tile, carry):
            held = [None] * EY
            for y in range(EY):
                rows = pl.ds(pl.multiple_of(8 * tile + EZ * y, 8), 8)
                parts = weights(swept[half, rows], scale * moved[1, rows, lanes])
                for target in range(max(y - 6, 0), min(y + 1, FY)):
                    part = parts[target - y + 6]
                    held[target] = part if held[target] is None else held[target] + part
                if y >= 6:
                    slots = pl.ds(pl.multiple_of(8 * tile + EZ * (y - 6), 8), 8)
                    landed[half, slots] = held[y - 6]
            return carry

        lax.fori_loop(0, EZ // 8, along_y, 0)

    def along_z(y, carry):
        for half in range(2):
            lanes = pl.ds(128 * half, 128)
            here = pl.ds(pl.multiple_of(EZ * y, 8), EZ)
            there = pl.ds(pl.multiple_of(EZ * (y + 3), 8), EZ)
            parts = weights(landed[half, here], scale * moved[2, there, lanes])
            total = parts[3][:FZ]
            for k, offset in enumerate((-3, -2, -1, 1, 2, 3)):
                part = parts[3 + offset]
                room = shifts.at[half, k]
                room[8:24, :] = part[:FZ]
                if offset > 0:
                    room[0:8, :] = part[FZ:]
                else:
                    room[24:32, :] = part[FZ:]
                total = total + room[pl.ds(8 - offset, FZ), :]
            out[y, :, lanes] = total
        return carry

    lax.fori_loop(0, FY, along_z, 0)


def shards(vorticity, scalar):
    lines, block = refine_tables()
    tables = [jnp.asarray(t) for t in spectral_tables() + (lines,)]
    tables.append(jnp.asarray(block, jnp.bfloat16))
    vmem = pl.BlockSpec(memory_space=pltpu.VMEM)
    f32 = jnp.float32
    operands = [vorticity.reshape(3, YB * ZB, N), scalar] + tables
    moved, ext, peak = pl.pallas_call(
        spectral_kernel,
        out_shape=(
            pltpu.VMEM((3, EY, EZ, 256), f32),
            pltpu.VMEM((EY, EZ, 256), f32),
            pltpu.VMEM((8, 128), f32),
        ),
        in_specs=[pl.BlockSpec(memory_space=pltpu.HBM)] * len(operands),
        out_specs=(vmem, vmem, vmem),
        scratch_shapes=[
            pltpu.VMEM((3, 128, 128), f32),
            *[pltpu.VMEM(t.shape, t.dtype) for t in tables],
            pltpu.VMEM((3, 2, 64, 128), f32),
            pltpu.VMEM((3, 2, 64, 128), f32),
            pltpu.VMEM((3, 128, 128), f32),
            pltpu.VMEM((3, 128, 128), f32),
            pltpu.VMEM((3, 128, 128), f32),
            pltpu.VMEM((3, 128, 128), f32),
            pltpu.VMEM((3, 2, 64, 128), f32),
            pltpu.VMEM((3, 2, 64, 128), f32),
            pltpu.VMEM((3, 256, 128), f32),
            pltpu.VMEM((3, 96, 128), f32),
            pltpu.VMEM((128, 128), f32),
            pltpu.SemaphoreType.DMA((12,)),
            pltpu.SemaphoreType.DMA((5,)),
            pltpu.SemaphoreType.DMA((5,)),
            pltpu.SemaphoreType.DMA((8,)),
            pltpu.SemaphoreType.DMA((8,)),
            pltpu.SemaphoreType.DMA((8,)),
            pltpu.SemaphoreType.DMA((8,)),
        ],
        compiler_params=pltpu.CompilerParams(
            collective_id=0, has_side_effects=True, vmem_limit_bytes=VMEM_LIMIT
        ),
        name="spectral",
    )(*[pltpu.with_memory_space_constraint(a, pltpu.HBM) for a in operands])
    return pl.pallas_call(
        remesh_kernel,
        out_shape=jax.ShapeDtypeStruct((FY, FZ, 256), f32),
        in_specs=[vmem] * 3,
        out_specs=vmem,
        scratch_shapes=[
            pltpu.VMEM((2, EY * EZ, 128), f32),
            pltpu.VMEM((2, FY * EZ, 128), f32),
            pltpu.VMEM((2, 6, 32, 128), f32),
        ],
        compiler_params=pltpu.CompilerParams(vmem_limit_bytes=VMEM_LIMIT),
        name="remesh",
    )(moved.reshape(3, EY * EZ, 256), ext.reshape(EY * EZ, 256), peak)


def solution(mesh):
    return jax.shard_map(
        shards,
        mesh=mesh,
        in_specs=(P(None, "row", "col", None), P("row", "col", None)),
        out_specs=P("row", "col", None),
        check_vma=False,
    )
```

```python
import functools
import math

import jax
import jax.numpy as jnp
import numpy as np
from jax import lax
from jax.experimental import pallas as pl
from jax.experimental.pallas import tpu as pltpu
from jax.sharding import PartitionSpec as P

COURANT = 0.9
EPSILON = 1e-06
VMEM_LIMIT = 24 << 20
MESH = pl.DeviceIdType.MESH
HIGH = lax.Precision.HIGH

N = 128
ROWS, COLS = 8, 16
CHIPS = 64
YB, ZB = 16, 8
FY, FZ = 32, 16
STEP = 19
EY, EZ = 38, 24


def turn(exponent):
    angle = 2.0 * math.pi * np.asarray(exponent, np.float64)
    return np.cos(angle), np.sin(angle)


def left_block(re, im):
    return np.block([[re, -im], [im, re]]).astype(np.float32)


def right_block(re, im):
    return np.block([[re, im], [-im, re]]).astype(np.float32)


@functools.cache
def spectral_tables():
    x = np.arange(N)
    k = np.arange(N // 2)
    cos, sin = turn(k[:, None] * x[None, :] / N)
    forward_x = np.concatenate([cos, -sin]).astype(np.float32)
    weight = np.where(k == 0, 1.0, 2.0)[:, None]
    inverse_x = np.concatenate([weight * cos, -weight * sin]).astype(np.float32)
    high = np.arange(64) // 8
    low = np.arange(64) % 8
    grid = (high[:, None] * high[None, :] + low[:, None] * low[None, :]) / 8.0
    forward_left, inverse_left = [], []
    for core in range(2):
        shift = low * (1 - core) / 16.0
        forward_left.append(left_block(*turn(-(grid + shift[:, None]))))
        inverse_left.append(left_block(*turn(grid + shift[None, :])))
    lane = np.arange(N)
    lane_y, lane_z = lane // 8, lane % 8
    lanes = lane_y[:, None] * lane_y[None, :] / 16.0 + lane_z[:, None] * lane_z[None, :] / 8.0
    forward_right = right_block(*turn(-lanes))
    inverse_right = right_block(*turn(lanes))
    twiddle = []
    waves = []
    for core in range(2):
        phase = high[:, None] * lane_y[None, :] + (low + 8 * core)[:, None] * lane_z[None, :]
        twiddle.append(np.stack(turn(-phase / N)))
        ky = high[:, None] + 8 * lane_y[None, :]
        kz = (low + 8 * core)[:, None] + 16 * lane_z[None, :]
        waves.append(np.stack([np.where(q < N // 2, q, q - N) for q in (ky, kz)]))
    return (
        forward_x,
        np.stack(forward_left),
        np.stack(twiddle).astype(np.float32),
        forward_right,
        np.stack(waves).astype(np.float32),
        inverse_right,
        np.stack(inverse_left),
        inverse_x,
    )


@functools.cache
def refine_tables():
    lines = np.zeros((N, 2 * N))
    for fine in range(2 * N):
        coarse = fine // 2
        lines[coarse, fine] += 0.75
        lines[(coarse + (1 if fine % 2 else -1)) % N, fine] += 0.25
    place = {}
    for y in range(YB):
        for z in range(ZB):
            place[y, z] = y * ZB + z
    for i in range(2):
        for z in range(ZB):
            place[i - 2, z] = 128 + i * ZB + z
            place[YB + i, z] = 144 + i * ZB + z
        for y in range(YB):
            place[y, i - 2] = 160 + i * YB + y
            place[y, ZB + i] = 192 + i * YB + y
    for index, (ys, zs) in enumerate(((-2, -2), (-2, ZB), (YB, -2), (YB, ZB))):
        for i in range(2):
            for j in range(2):
                place[ys + j, zs + i] = 224 + 8 * index + 2 * i + j

    def taps(fine):
        coarse = fine // 2
        return ((coarse, 0.75), (coarse + (1 if fine % 2 else -1), 0.25))

    slots = list(range(FZ)) + [16, 17, 18, None, None, -3, -2, -1]
    block = np.zeros((EY * EZ, 256))
    for row in range(EY):
        for slot, fine_z in enumerate(slots):
            if fine_z is None:
                continue
            for y, wy in taps(row - 3):
                for z, wz in taps(fine_z):
                    block[row * EZ + slot, place[y, z]] += wy * wz
    return lines.astype(np.float32), block.astype(np.float32)


def dot(a, b, contract=(1, 0)):
    return lax.dot_general(
        a,
        b,
        (((contract[0],), (contract[1],)), ((), ())),
        precision=HIGH,
        preferred_element_type=jnp.float32,
    )


FAR_FIRST = sorted(
    ((dx, dy, dz) for dx in range(4) for dy in range(4) for dz in range(4)),
    key=lambda d: -sum(min(step, 4 - step) for step in d),
)


def spectral_kernel(
    vort_hbm,
    scal,
    *refs,
):
    table_hbm, (moved_out, wide_out, ext_out, peak_out), refs = refs[:10], refs[10:14], refs[14:]
    vort, tables, refs = refs[0], refs[1:11], refs[11:]
    fwd_x, fwd_left, twiddle, fwd_right, waves, inv_right, inv_left, inv_x, lines, block = tables
    s_buf, r_buf, z_buf, zo_buf, y_buf, yo_buf, t_buf, u_buf, rim, pieces, peaks = refs[:11]
    load_sem, send_sem, recv_sem, swap_send, swap_recv = refs[11:16]
    scal_send, scal_recv, rim_send, rim_recv = refs[16:]

    row = lax.axis_index("row")
    col = lax.axis_index("col")
    core = lax.rem(col, 2)
    half = lax.div(col, 2)
    chip = row * 8 + half
    other = 1 - core
    up_row, down_row = lax.rem(row + 1, ROWS), lax.rem(row + ROWS - 1, ROWS)
    up_col, down_col = lax.rem(col + 1, COLS), lax.rem(col + COLS - 1, COLS)

    loads = [pltpu.make_async_copy(vort_hbm, vort, load_sem.at[0])]
    for i in range(10):
        loads.append(pltpu.make_async_copy(table_hbm[i], tables[i], load_sem.at[1 + i]))
    loads.append(
        pltpu.make_async_copy(
            scal, ext_out.at[pl.ds(3, FY), pl.ds(0, FZ), :], load_sem.at[11]
        )
    )
    for load in loads[:2] + loads[11:] + loads[2:11]:
        load.start()

    y0, x0 = lax.rem(row, 4), lax.rem(half, 4)
    z0 = 2 * lax.div(half, 4) + lax.div(row, 4)
    xs = [lax.rem(x0 + d, 4) for d in range(4)]
    ys = [lax.rem(y0 + d, 4) for d in range(4)]
    zs = [lax.rem(z0 + d, 4) for d in range(4)]
    low = [4 * lax.rem(z, 2) for z in zs]
    high = [4 * lax.div(z, 2) for z in zs]
    to_rows = [[low[dz] + ys[dy] for dz in range(4)] for dy in range(4)]
    to_halves = [[high[dz] + xs[dx] for dz in range(4)] for dx in range(4)]
    chips = [(to_rows[dy][dz], to_halves[dx][dz]) for dx, dy, dz in FAR_FIRST]
    devices = [(r, 2 * h + c) for r, h in chips for c in (other, core)][:-1]

    barrier = pltpu.get_barrier_semaphore()
    for device in devices:
        pl.semaphore_signal(barrier, inc=1, device_id=device, device_id_type=MESH)

    loads[0].wait()
    loads[1].wait()
    for c in range(3):
        s_buf[c] = dot(fwd_x[...], vort[c], (1, 1)).reshape(2, 64, 128)
    pieces[...] = jnp.zeros_like(pieces)
    for load in loads[2:]:
        load.wait()
    pl.semaphore_wait(barrier, 2 * CHIPS - 1)

    def exchange(source, target, index):
        for to_row, to_half in chips:
            pltpu.make_async_remote_copy(
                src_ref=source.at[:, :, pl.ds(to_row * 8 + to_half, 1), :],
                dst_ref=target.at[:, :, pl.ds(chip, 1), :],
                send_sem=send_sem.at[index],
                recv_sem=recv_sem.at[index],
                device_id=(to_row, 2 * to_half + other),
                device_id_type=MESH,
            ).start()

    def swap(source, target, index, c):
        copy = pltpu.make_async_remote_copy(
            src_ref=source.at[c],
            dst_ref=target.at[c],
            send_sem=swap_send.at[index, c],
            recv_sem=swap_recv.at[index, c],
            device_id=(row, col + 1 - 2 * core),
            device_id_type=MESH,
        )
        copy.start()
        return copy

    def arrive(target, index):
        pltpu.make_async_copy(target, target, recv_sem.at[index]).wait()

    def left(source, index):
        pltpu.make_async_copy(source, source, send_sem.at[index]).wait()

    exchange(s_buf, r_buf, 0)

    def scal_copy(i, ys, zs, yt, zt, device):
        return pltpu.make_async_remote_copy(
            src_ref=ext_out.at[pl.ds(*ys), pl.ds(*zs), :],
            dst_ref=ext_out.at[pl.ds(*yt), pl.ds(*zt), :],
            send_sem=scal_send.at[i],
            recv_sem=scal_recv.at[i],
            device_id=device,
            device_id_type=MESH,
        )

    y_first, y_last, y_below, y_above, y_all = (3, 3), (32, 3), (0, 3), (35, 3), (3, FY)
    z_first, z_last, z_below, z_above, z_all = (0, 3), (13, 3), (21, 3), (16, 3), (0, FZ)
    scal_copies = [
        scal_copy(0, y_first, z_all, y_above, z_all, (down_row, col)),
        scal_copy(1, y_last, z_all, y_below, z_all, (up_row, col)),
        scal_copy(2, y_all, z_first, y_all, z_above, (row, down_col)),
        scal_copy(3, y_all, z_last, y_all, z_below, (row, up_col)),
        scal_copy(4, y_first, z_first, y_above, z_above, (down_row, down_col)),
        scal_copy(5, y_first, z_last, y_above, z_below, (down_row, up_col)),
        scal_copy(6, y_last, z_first, y_below, z_above, (up_row, down_col)),
        scal_copy(7, y_last, z_last, y_below, z_below, (up_row, up_col)),
    ]
    for copy in scal_copies:
        copy.start()

    arrive(r_buf, 0)
    swaps = []
    for c in range(3):
        z_buf[c] = dot(fwd_left[core], r_buf[c].reshape(128, 128))
        swaps.append(swap(z_buf, zo_buf, 0, c))
    sign = (1 - 2 * core).astype(jnp.float32)
    tw_re = twiddle[core, 0]
    tw_im = twiddle[core, 1]
    ky = waves[core, 0]
    kz = waves[core, 1]
    kx = chip.astype(jnp.float32)
    k_sq = kx * kx + ky * ky + kz * kz
    keep = (k_sq > 0.0) & (ky > -64.0) & (kz > -64.0)
    factor = jnp.where(keep, 1.0 / jnp.maximum(k_sq, 1.0), 0.0) * (1.0 / (N * N * N))
    omega = []
    for c in range(3):
        swaps[c].wait_recv()
        joined = z_buf[c] + sign * zo_buf[c]
        re, im = joined[:64], joined[64:]
        pair = jnp.concatenate([re * tw_re - im * tw_im, re * tw_im + im * tw_re], axis=1)
        spectrum = dot(pair, fwd_right[...])
        omega.append((spectrum[:, :128], spectrum[:, 128:]))

    def cross(part):
        w0, w1, w2 = omega[0][part], omega[1][part], omega[2][part]
        return (ky * w2 - kz * w1, kz * w0 - kx * w2, kx * w1 - ky * w0)

    cross_re, cross_im = cross(0), cross(1)
    for c in range(3):
        pair = jnp.concatenate([-cross_im[c] * factor, cross_re[c] * factor], axis=1)
        back = dot(pair, inv_right[...])
        re, im = back[:, :128], back[:, 128:]
        y_buf[c, :64] = re * tw_re + im * tw_im
        y_buf[c, 64:] = im * tw_re - re * tw_im
        swaps.append(swap(y_buf, yo_buf, 1, c))
    for c in range(3):
        swaps[3 + c].wait_recv()
        joined = y_buf[c] - sign * yo_buf[c]
        t_buf[c] = dot(inv_left[core], joined).reshape(2, 64, 128)
    exchange(t_buf, u_buf, 1)
    arrive(u_buf, 1)
    top = jnp.zeros((8, 128), jnp.float32)
    for c in range(3):
        velocity = dot(u_buf[c].reshape(128, 128), inv_x[...], (0, 0))
        rim[c, :128] = velocity
        top = jnp.maximum(top, jnp.max(jnp.abs(velocity).reshape(16, 8, 128), axis=0))
    mine = row * COLS + col
    peaks[pl.ds(mine, 1), :] = jnp.max(top, axis=0, keepdims=True)
    for c in range(3):
        for i in range(2):
            pieces[c, pl.ds(16 * i, 16), :] = rim[c, pl.ds(6 + i, 16, 8), :]
            pieces[c, pl.ds(32 + 16 * i, 16), :] = rim[c, pl.ds(i, 16, 8), :]
            for index, (y, z) in enumerate(((14, 6), (14, 0), (0, 6), (0, 0))):
                pieces[c, pl.ds(64 + 8 * index + 2 * i, 2), :] = rim[
                    c, pl.ds(8 * y + z + i, 2, 8), :
                ]

    def rim_copy(i, source, start, target, count, device):
        return pltpu.make_async_remote_copy(
            src_ref=source.at[:, pl.ds(start, count), :],
            dst_ref=rim.at[:, pl.ds(target, count), :],
            send_sem=rim_send.at[i],
            recv_sem=rim_recv.at[i],
            device_id=device,
            device_id_type=MESH,
        )

    rim_copies = [
        rim_copy(0, rim, 112, 128, 16, (up_row, col)),
        rim_copy(1, rim, 0, 144, 16, (down_row, col)),
        rim_copy(2, pieces, 0, 160, 32, (row, up_col)),
        rim_copy(3, pieces, 32, 192, 32, (row, down_col)),
        rim_copy(4, pieces, 64, 224, 8, (up_row, up_col)),
        rim_copy(5, pieces, 72, 232, 8, (up_row, down_col)),
        rim_copy(6, pieces, 80, 240, 8, (down_row, up_col)),
        rim_copy(7, pieces, 88, 248, 8, (down_row, down_col)),
    ]
    for copy in rim_copies:
        copy.start()
    for device in devices:
        pltpu.make_async_remote_copy(
            src_ref=peaks.at[pl.ds(mine, 1), :],
            dst_ref=peaks.at[pl.ds(mine, 1), :],
            send_sem=send_sem.at[2],
            recv_sem=recv_sem.at[2],
            device_id=device,
            device_id_type=MESH,
        ).start()
    for copy in rim_copies:
        copy.wait_recv()
    for c in range(3):
        wide = dot(rim[c], lines[...])
        big = wide.astype(jnp.bfloat16)
        small = (wide - big.astype(jnp.float32)).astype(jnp.bfloat16)
        if c == 0:
            moved_out[...] = refine(block[...], big, small)
        else:
            wide_out[2 * c - 2] = big
            wide_out[2 * c - 1] = small
    others = peaks.at[pl.ds(0, 2 * CHIPS - 1), :]
    arrive(others, 2)
    peak_out[...] = jnp.max(peaks[...].reshape(16, 8, 128), axis=0)
    for copy in scal_copies:
        copy.wait_recv()
    left(s_buf, 0)
    left(t_buf, 1)
    left(others, 2)
    for copy in swaps + scal_copies + rim_copies:
        copy.wait_send()


def refine(block, big, small):
    fine = jnp.dot(block, big, preferred_element_type=jnp.float32)
    return fine + jnp.dot(block, small, preferred_element_type=jnp.float32)


def weights(field, moved):
    size = jnp.abs(moved)
    square = moved * moved
    first = field * moved
    second = first * moved
    core = second * (7.0 / 48.0 - size * (0.25 - (5.0 / 48.0) * size))
    even3 = core * size
    odd3 = core * moved
    bend = first * (square * (1.0 / 24.0) - 1.0 / 24.0)
    even2 = bend * moved - 6.0 * even3
    odd2 = (bend + bend) - 4.0 * odd3
    even1 = 0.5 * second - 4.0 * even2 - 9.0 * even3
    odd1 = 0.5 * first - (odd2 + odd2) - 3.0 * odd3
    side = even1 + even2 + even3
    return (
        even3 - odd3,
        even2 - odd2,
        even1 - odd1,
        field - (side + side),
        even1 + odd1,
        even2 + odd2,
        even3 + odd3,
    )


def sweep_roll(field, moved, axis):
    parts = weights(field, moved)
    length = field.shape[axis]
    total = parts[3]
    for offset in (-3, -2, -1, 1, 2, 3):
        total = total + pltpu.roll(parts[3 + offset], offset % length, axis)
    return total


def remesh_kernel(moved, wide, ext, peak, block, out, later, swept, landed, shifts):
    top = jnp.max(peak[...], axis=1, keepdims=True)
    top = jnp.max(top, axis=0, keepdims=True)
    scale = COURANT / (top + EPSILON)

    def along_x(i, carry):
        span = pl.ds(pl.multiple_of(8 * STEP * i, 8), 8 * STEP)
        for c in range(2):
            later[c, span] = refine(block[span], wide[2 * c], wide[2 * c + 1])
        for tile in range(STEP):
            rows = pl.ds(pl.multiple_of(8 * (STEP * i + tile), 8), 8)
            total = sweep_roll(ext[rows], scale * moved[rows], 1)
            swept[0, rows] = total[:, :128]
            swept[1, rows] = total[:, 128:]
        return carry

    lax.fori_loop(0, EY * EZ // 8 // STEP, along_x, 0)
    for half in range(2):
        lanes = pl.ds(128 * half, 128)

        def along_y(tile, carry):
            held = [None] * EY
            for y in range(EY):
                rows = pl.ds(pl.multiple_of(8 * tile + EZ * y, 8), 8)
                parts = weights(swept[half, rows], scale * later[0, rows, lanes])
                for target in range(max(y - 6, 0), min(y + 1, FY)):
                    part = parts[target - y + 6]
                    held[target] = part if held[target] is None else held[target] + part
                if y >= 6:
                    slots = pl.ds(pl.multiple_of(8 * tile + EZ * (y - 6), 8), 8)
                    landed[half, slots] = held[y - 6]
            return carry

        lax.fori_loop(0, EZ // 8, along_y, 0)

    def along_z(y, carry):
        for half in range(2):
            lanes = pl.ds(128 * half, 128)
            here = pl.ds(pl.multiple_of(EZ * y, 8), EZ)
            there = pl.ds(pl.multiple_of(EZ * (y + 3), 8), EZ)
            parts = weights(landed[half, here], scale * later[1, there, lanes])
            total = parts[3][:FZ]
            for k, offset in enumerate((-3, -2, -1, 1, 2, 3)):
                part = parts[3 + offset]
                room = shifts.at[half, k]
                room[8:24, :] = part[:FZ]
                if offset > 0:
                    room[0:8, :] = part[FZ:]
                else:
                    room[24:32, :] = part[FZ:]
                total = total + room[pl.ds(8 - offset, FZ), :]
            out[y, :, lanes] = total
        return carry

    lax.fori_loop(0, FY, along_z, 0)


def shards(vorticity, scalar):
    lines, block = refine_tables()
    tables = [jnp.asarray(t) for t in spectral_tables() + (lines,)]
    tables.append(jnp.asarray(block, jnp.bfloat16))
    vmem = pl.BlockSpec(memory_space=pltpu.VMEM)
    f32 = jnp.float32
    operands = [vorticity.reshape(3, YB * ZB, N), scalar] + tables
    moved, wide, ext, peak = pl.pallas_call(
        spectral_kernel,
        out_shape=(
            pltpu.VMEM((EY * EZ, 256), f32),
            pltpu.VMEM((4, 256, 256), jnp.bfloat16),
            pltpu.VMEM((EY, EZ, 256), f32),
            pltpu.VMEM((8, 128), f32),
        ),
        in_specs=[pl.BlockSpec(memory_space=pltpu.HBM)] * len(operands),
        out_specs=(vmem,) * 4,
        scratch_shapes=[
            pltpu.VMEM((3, 128, 128), f32),
            *[pltpu.VMEM(t.shape, t.dtype) for t in tables],
            pltpu.VMEM((3, 2, 64, 128), f32),
            pltpu.VMEM((3, 2, 64, 128), f32),
            pltpu.VMEM((3, 128, 128), f32),
            pltpu.VMEM((3, 128, 128), f32),
            pltpu.VMEM((3, 128, 128), f32),
            pltpu.VMEM((3, 128, 128), f32),
            pltpu.VMEM((3, 2, 64, 128), f32),
            pltpu.VMEM((3, 2, 64, 128), f32),
            pltpu.VMEM((3, 256, 128), f32),
            pltpu.VMEM((3, 96, 128), f32),
            pltpu.VMEM((128, 128), f32),
            pltpu.SemaphoreType.DMA((12,)),
            pltpu.SemaphoreType.DMA((3,)),
            pltpu.SemaphoreType.DMA((3,)),
            pltpu.SemaphoreType.DMA((2, 3)),
            pltpu.SemaphoreType.DMA((2, 3)),
            pltpu.SemaphoreType.DMA((8,)),
            pltpu.SemaphoreType.DMA((8,)),
            pltpu.SemaphoreType.DMA((8,)),
            pltpu.SemaphoreType.DMA((8,)),
        ],
        compiler_params=pltpu.CompilerParams(
            collective_id=0, has_side_effects=True, vmem_limit_bytes=VMEM_LIMIT
        ),
        name="spectral",
    )(*[pltpu.with_memory_space_constraint(a, pltpu.HBM) for a in operands])
    return pl.pallas_call(
        remesh_kernel,
        out_shape=jax.ShapeDtypeStruct((FY, FZ, 256), f32),
        in_specs=[vmem] * 5,
        out_specs=vmem,
        scratch_shapes=[
            pltpu.VMEM((2, EY * EZ, 256), f32),
            pltpu.VMEM((2, EY * EZ, 128), f32),
            pltpu.VMEM((2, FY * EZ, 128), f32),
            pltpu.VMEM((2, 6, 32, 128), f32),
        ],
        compiler_params=pltpu.CompilerParams(vmem_limit_bytes=VMEM_LIMIT),
        name="remesh",
    )(moved, wide, ext.reshape(EY * EZ, 256), peak, tables[-1])


def solution(mesh):
    return jax.shard_map(
        shards,
        mesh=mesh,
        in_specs=(P(None, "row", "col", None), P("row", "col", None)),
        out_specs=P("row", "col", None),
        check_vma=False,
    )
```

```python
import functools
import math

import jax
import jax.numpy as jnp
import numpy as np
from jax import lax
from jax.experimental import pallas as pl
from jax.experimental.pallas import tpu as pltpu
from jax.sharding import PartitionSpec as P

COURANT = 0.9
EPSILON = 1e-06
VMEM_LIMIT = 24 << 20
MESH = pl.DeviceIdType.MESH
HIGH = lax.Precision.HIGH

N = 128
ROWS, COLS = 8, 16
CHIPS = 64
YB, ZB = 16, 8
FY, FZ = 32, 16
LINES = 8
STEP = 57
EY, EZ = 38, 24


def turn(exponent):
    angle = 2.0 * math.pi * np.asarray(exponent, np.float64)
    return np.cos(angle), np.sin(angle)


def left_block(re, im):
    return np.block([[re, -im], [im, re]]).astype(np.float32)


def right_block(re, im):
    return np.block([[re, im], [-im, re]]).astype(np.float32)


@functools.cache
def spectral_tables():
    x = np.arange(N)
    k = np.arange(N // 2)
    cos, sin = turn(k[:, None] * x[None, :] / N)
    forward_x = np.concatenate([cos, -sin]).astype(np.float32)
    weight = np.where(k == 0, 1.0, 2.0)[:, None]
    inverse_x = np.concatenate([weight * cos, -weight * sin]).astype(np.float32)
    high = np.arange(64) // 8
    low = np.arange(64) % 8
    grid = (high[:, None] * high[None, :] + low[:, None] * low[None, :]) / 8.0
    forward_left, inverse_left = [], []
    for core in range(2):
        shift = low * (1 - core) / 16.0
        forward_left.append(left_block(*turn(-(grid + shift[:, None]))))
        inverse_left.append(left_block(*turn(grid + shift[None, :])))
    lane = np.arange(N)
    lane_y, lane_z = lane // 8, lane % 8
    lanes = lane_y[:, None] * lane_y[None, :] / 16.0 + lane_z[:, None] * lane_z[None, :] / 8.0
    forward_right = right_block(*turn(-lanes))
    inverse_right = right_block(*turn(lanes))
    twiddle = []
    waves = []
    for core in range(2):
        phase = high[:, None] * lane_y[None, :] + (low + 8 * core)[:, None] * lane_z[None, :]
        twiddle.append(np.stack(turn(-phase / N)))
        ky = high[:, None] + 8 * lane_y[None, :]
        kz = (low + 8 * core)[:, None] + 16 * lane_z[None, :]
        waves.append(np.stack([np.where(q < N // 2, q, q - N) for q in (ky, kz)]))
    return (
        forward_x,
        np.stack(forward_left),
        np.stack(twiddle).astype(np.float32),
        forward_right,
        np.stack(waves).astype(np.float32),
        inverse_right,
        np.stack(inverse_left),
        inverse_x,
    )


@functools.cache
def refine_tables():
    lines = np.zeros((N, 2 * N))
    for fine in range(2 * N):
        coarse = fine // 2
        lines[coarse, fine] += 0.75
        lines[(coarse + (1 if fine % 2 else -1)) % N, fine] += 0.25
    place = {}
    for y in range(YB):
        for z in range(ZB):
            place[y, z] = y * ZB + z
    for i in range(2):
        for z in range(ZB):
            place[i - 2, z] = 128 + i * ZB + z
            place[YB + i, z] = 144 + i * ZB + z
        for y in range(YB):
            place[y, i - 2] = 160 + i * YB + y
            place[y, ZB + i] = 192 + i * YB + y
    for index, (ys, zs) in enumerate(((-2, -2), (-2, ZB), (YB, -2), (YB, ZB))):
        for i in range(2):
            for j in range(2):
                place[ys + j, zs + i] = 224 + 8 * index + 2 * i + j

    def taps(fine):
        coarse = fine // 2
        return ((coarse, 0.75), (coarse + (1 if fine % 2 else -1), 0.25))

    slots = list(range(FZ)) + [16, 17, 18, None, None, -3, -2, -1]
    block = np.zeros((EY * EZ, 256))
    for row in range(EY):
        for slot, fine_z in enumerate(slots):
            if fine_z is None:
                continue
            for y, wy in taps(row - 3):
                for z, wz in taps(fine_z):
                    block[row * EZ + slot, place[y, z]] += wy * wz
    order = np.concatenate([np.arange(0, 2 * N, 2), np.arange(1, 2 * N, 2)])
    return lines[:, order].astype(np.float32), block.astype(np.float32), np.eye(2 * N)[:, order]


def dot(a, b, contract=(1, 0)):
    return lax.dot_general(
        a,
        b,
        (((contract[0],), (contract[1],)), ((), ())),
        precision=HIGH,
        preferred_element_type=jnp.float32,
    )


FAR_FIRST = sorted(
    ((dx, dy, dz) for dx in range(4) for dy in range(4) for dz in range(4)),
    key=lambda d: -sum(min(step, 4 - step) for step in d),
)


def side_by_side(parts):
    return jnp.concatenate(parts, axis=1)


def spectral_kernel(
    vort_hbm,
    scal,
    *refs,
):
    table_hbm, (moved_out, wide_out, ext_out, peak_out), refs = refs[:11], refs[11:15], refs[15:]
    vort, stage, tables, refs = refs[0], refs[1], refs[2:13], refs[13:]
    fwd_x, fwd_left, twiddle, fwd_right, waves, inv_right, inv_left, inv_x = tables[:8]
    lines, block, parity = tables[8:]
    s_buf, r_buf, z_buf, zo_buf, y_buf, yo_buf, t_buf, u_buf, rim, pieces, peaks = refs[:11]
    load_sem, send_sem, recv_sem, swap_send, swap_recv = refs[11:16]
    scal_send, scal_recv, rim_send, rim_recv = refs[16:]

    row = lax.axis_index("row")
    col = lax.axis_index("col")
    core = lax.rem(col, 2)
    half = lax.div(col, 2)
    chip = row * 8 + half
    other = 1 - core
    up_row, down_row = lax.rem(row + 1, ROWS), lax.rem(row + ROWS - 1, ROWS)
    up_col, down_col = lax.rem(col + 1, COLS), lax.rem(col + COLS - 1, COLS)

    loads = [pltpu.make_async_copy(vort_hbm, vort, load_sem.at[0])]
    for i in range(11):
        loads.append(pltpu.make_async_copy(table_hbm[i], tables[i], load_sem.at[1 + i]))
    loads.append(pltpu.make_async_copy(scal, stage, load_sem.at[12]))
    for load in loads:
        load.start()

    y0, x0 = lax.rem(row, 4), lax.rem(half, 4)
    z0 = 2 * lax.div(half, 4) + lax.div(row, 4)
    xs = [lax.rem(x0 + d, 4) for d in range(4)]
    ys = [lax.rem(y0 + d, 4) for d in range(4)]
    zs = [lax.rem(z0 + d, 4) for d in range(4)]
    low = [4 * lax.rem(z, 2) for z in zs]
    high = [4 * lax.div(z, 2) for z in zs]
    to_rows = [[low[dz] + ys[dy] for dz in range(4)] for dy in range(4)]
    to_halves = [[high[dz] + xs[dx] for dz in range(4)] for dx in range(4)]
    chips = [(to_rows[dy][dz], to_halves[dx][dz]) for dx, dy, dz in FAR_FIRST]
    devices = [(r, 2 * h + c) for r, h in chips for c in (other, core)][:-1]

    barrier = pltpu.get_barrier_semaphore()
    for device in devices:
        pl.semaphore_signal(barrier, inc=1, device_id=device, device_id_type=MESH)

    loads[0].wait()
    loads[1].wait()
    for c in range(3):
        s_buf[c] = dot(fwd_x[...], vort[c], (1, 1)).reshape(2, 64, 128)
    pieces[...] = jnp.zeros_like(pieces)
    for load in loads[2:]:
        load.wait()
    pl.semaphore_wait(barrier, 2 * CHIPS - 1)

    def exchange(source, target, index):
        for to_row, to_half in chips:
            pltpu.make_async_remote_copy(
                src_ref=source.at[:, :, pl.ds(to_row * 8 + to_half, 1), :],
                dst_ref=target.at[:, :, pl.ds(chip, 1), :],
                send_sem=send_sem.at[index],
                recv_sem=recv_sem.at[index],
                device_id=(to_row, 2 * to_half + other),
                device_id_type=MESH,
            ).start()

    def swap(source, target, index, c):
        copy = pltpu.make_async_remote_copy(
            src_ref=source.at[c],
            dst_ref=target.at[c],
            send_sem=swap_send.at[index, c],
            recv_sem=swap_recv.at[index, c],
            device_id=(row, col + 1 - 2 * core),
            device_id_type=MESH,
        )
        copy.start()
        return copy

    def arrive(target, index):
        pltpu.make_async_copy(target, target, recv_sem.at[index]).wait()

    def left(source, index):
        pltpu.make_async_copy(source, source, send_sem.at[index]).wait()

    exchange(s_buf, r_buf, 0)

    held = stage[...].reshape(FY * FZ, 256)
    total = jnp.zeros((FY * FZ, 256), jnp.float32)
    for _ in range(3):
        piece = held.astype(jnp.bfloat16)
        held = held - piece.astype(jnp.float32)
        total = total + jnp.dot(piece, parity[...], preferred_element_type=jnp.float32)
    ext_out[pl.ds(3, FY), pl.ds(0, FZ), :] = total.reshape(FY, FZ, 256)

    def scal_copy(i, ys, zs, yt, zt, device):
        return pltpu.make_async_remote_copy(
            src_ref=ext_out.at[pl.ds(*ys), pl.ds(*zs), :],
            dst_ref=ext_out.at[pl.ds(*yt), pl.ds(*zt), :],
            send_sem=scal_send.at[i],
            recv_sem=scal_recv.at[i],
            device_id=device,
            device_id_type=MESH,
        )

    y_first, y_last, y_below, y_above, y_all = (3, 3), (32, 3), (0, 3), (35, 3), (3, FY)
    z_first, z_last, z_below, z_above, z_all = (0, 3), (13, 3), (21, 3), (16, 3), (0, FZ)
    scal_copies = [
        scal_copy(0, y_first, z_all, y_above, z_all, (down_row, col)),
        scal_copy(1, y_last, z_all, y_below, z_all, (up_row, col)),
        scal_copy(2, y_all, z_first, y_all, z_above, (row, down_col)),
        scal_copy(3, y_all, z_last, y_all, z_below, (row, up_col)),
        scal_copy(4, y_first, z_first, y_above, z_above, (down_row, down_col)),
        scal_copy(5, y_first, z_last, y_above, z_below, (down_row, up_col)),
        scal_copy(6, y_last, z_first, y_below, z_above, (up_row, down_col)),
        scal_copy(7, y_last, z_last, y_below, z_below, (up_row, up_col)),
    ]
    for copy in scal_copies:
        copy.start()

    arrive(r_buf, 0)
    swaps = []
    for c in range(3):
        z_buf[c] = dot(fwd_left[core], r_buf[c].reshape(128, 128))
        swaps.append(swap(z_buf, zo_buf, 0, c))
    sign = (1 - 2 * core).astype(jnp.float32)
    tw_re = twiddle[core, 0]
    tw_im = twiddle[core, 1]
    ky = waves[core, 0]
    kz = waves[core, 1]
    kx = chip.astype(jnp.float32)
    k_sq = kx * kx + ky * ky + kz * kz
    keep = (k_sq > 0.0) & (ky > -64.0) & (kz > -64.0)
    factor = jnp.where(keep, 1.0 / jnp.maximum(k_sq, 1.0), 0.0) * (1.0 / (N * N * N))
    for copy in swaps:
        copy.wait_recv()
    pairs = []
    for c in range(3):
        joined = z_buf[c] + sign * zo_buf[c]
        re, im = joined[:64], joined[64:]
        pairs.append(side_by_side([re * tw_re - im * tw_im, re * tw_im + im * tw_re]))
    spectrum = dot(jnp.concatenate(pairs), fwd_right[...])

    def cross(part):
        lanes = slice(128 * part, 128 * part + 128)
        w0, w1, w2 = spectrum[:64, lanes], spectrum[64:128, lanes], spectrum[128:, lanes]
        return (ky * w2 - kz * w1, kz * w0 - kx * w2, kx * w1 - ky * w0)

    cross_re, cross_im = cross(0), cross(1)
    pairs = [side_by_side([-cross_im[c] * factor, cross_re[c] * factor]) for c in range(3)]
    back = dot(jnp.concatenate(pairs), inv_right[...])
    for c in range(3):
        re, im = back[64 * c : 64 * c + 64, :128], back[64 * c : 64 * c + 64, 128:]
        y_buf[c, :64] = re * tw_re + im * tw_im
        y_buf[c, 64:] = im * tw_re - re * tw_im
        swaps.append(swap(y_buf, yo_buf, 1, c))
    for copy in swaps[3:]:
        copy.wait_recv()
    joined = dot(
        inv_left[core], side_by_side([y_buf[c] - sign * yo_buf[c] for c in range(3)])
    )
    for c in range(3):
        t_buf[c] = joined[:, 128 * c : 128 * c + 128].reshape(2, 64, 128)
    exchange(t_buf, u_buf, 1)
    arrive(u_buf, 1)
    top = jnp.zeros((8, 128), jnp.float32)
    joined = dot(
        side_by_side([u_buf[c].reshape(128, 128) for c in range(3)]), inv_x[...], (0, 0)
    )
    for c in range(3):
        velocity = joined[128 * c : 128 * c + 128]
        rim[c, :128] = velocity
        top = jnp.maximum(top, jnp.max(jnp.abs(velocity).reshape(16, 8, 128), axis=0))
    mine = row * COLS + col
    peaks[pl.ds(mine, 1), :] = jnp.max(top, axis=0, keepdims=True)

    def send_peaks(targets):
        for device in targets:
            pltpu.make_async_remote_copy(
                src_ref=peaks.at[pl.ds(mine, 1), :],
                dst_ref=peaks.at[pl.ds(mine, 1), :],
                send_sem=send_sem.at[2],
                recv_sem=recv_sem.at[2],
                device_id=device,
                device_id_type=MESH,
            ).start()

    send_peaks(devices[:32])
    for c in range(3):
        for i in range(2):
            pieces[c, pl.ds(16 * i, 16), :] = rim[c, pl.ds(6 + i, 16, 8), :]
            pieces[c, pl.ds(32 + 16 * i, 16), :] = rim[c, pl.ds(i, 16, 8), :]
            for index, (y, z) in enumerate(((14, 6), (14, 0), (0, 6), (0, 0))):
                pieces[c, pl.ds(64 + 8 * index + 2 * i, 2), :] = rim[
                    c, pl.ds(8 * y + z + i, 2, 8), :
                ]

    def rim_copy(i, source, start, target, count, device):
        return pltpu.make_async_remote_copy(
            src_ref=source.at[:, pl.ds(start, count), :],
            dst_ref=rim.at[:, pl.ds(target, count), :],
            send_sem=rim_send.at[i],
            recv_sem=rim_recv.at[i],
            device_id=device,
            device_id_type=MESH,
        )

    rim_copies = [
        rim_copy(0, rim, 112, 128, 16, (up_row, col)),
        rim_copy(1, rim, 0, 144, 16, (down_row, col)),
        rim_copy(2, pieces, 0, 160, 32, (row, up_col)),
        rim_copy(3, pieces, 32, 192, 32, (row, down_col)),
        rim_copy(4, pieces, 64, 224, 8, (up_row, up_col)),
        rim_copy(5, pieces, 72, 232, 8, (up_row, down_col)),
        rim_copy(6, pieces, 80, 240, 8, (down_row, up_col)),
        rim_copy(7, pieces, 88, 248, 8, (down_row, down_col)),
    ]
    for copy in rim_copies:
        copy.start()
    send_peaks(devices[32:])
    for copy in rim_copies:
        copy.wait_recv()
    for c in range(3):
        wide = dot(rim[c], lines[...])
        big = wide.astype(jnp.bfloat16)
        small = (wide - big.astype(jnp.float32)).astype(jnp.bfloat16)
        if c == 0:
            moved_out[...] = refine(block[...], big, small)
        else:
            wide_out[2 * c - 2] = big
            wide_out[2 * c - 1] = small
    others = peaks.at[pl.ds(0, 2 * CHIPS - 1), :]
    arrive(others, 2)
    peak_out[...] = jnp.max(peaks[...].reshape(16, 8, 128), axis=0)
    for copy in scal_copies:
        copy.wait_recv()
    left(s_buf, 0)
    left(t_buf, 1)
    left(others, 2)
    for copy in swaps + scal_copies + rim_copies:
        copy.wait_send()


def refine(block, big, small):
    fine = jnp.dot(block, big, preferred_element_type=jnp.float32)
    return fine + jnp.dot(block, small, preferred_element_type=jnp.float32)


def weights(field, moved):
    size = jnp.abs(moved)
    square = moved * moved
    first = field * moved
    second = first * moved
    core = second * (7.0 / 48.0 - size * (0.25 - (5.0 / 48.0) * size))
    even3 = core * size
    odd3 = core * moved
    bend = first * (square * (1.0 / 24.0) - 1.0 / 24.0)
    even2 = bend * moved - 6.0 * even3
    odd2 = (bend + bend) - 4.0 * odd3
    even1 = 0.5 * second - 4.0 * even2 - 9.0 * even3
    odd1 = 0.5 * first - (odd2 + odd2) - 3.0 * odd3
    side = even1 + even2 + even3
    return (
        even3 - odd3,
        even2 - odd2,
        even1 - odd1,
        field - (side + side),
        even1 + odd1,
        even2 + odd2,
        even3 + odd3,
    )


def sweep_x(even, odd, even_moved, odd_moved):
    e3, e2, e1, e, f1, f2, f3 = weights(even, even_moved)
    o3, o2, o1, o, p1, p2, p3 = weights(odd, odd_moved)

    def roll(a, shift):
        return pltpu.roll(a, shift % 128, 1)

    return (
        (e + o1) + roll(p1 + f2, 1) + roll(e2 + o3, -1) + roll(p3, 2),
        (o + f1) + roll(e1 + o2, -1) + roll(p2 + f3, 1) + roll(e3, -2),
    )


def remesh_kernel(moved, wide, ext, peak, block, out, later, swept, landed, shifts):
    top = jnp.max(peak[...], axis=1, keepdims=True)
    top = jnp.max(top, axis=0, keepdims=True)
    scale = COURANT / (top + EPSILON)

    def along_x(i, carry):
        span = pl.ds(pl.multiple_of(8 * STEP * i, 8), 8 * STEP)
        for c in range(2):
            later[c, span] = refine(block[span], wide[2 * c], wide[2 * c + 1])
        for tile in range(STEP):
            rows = pl.ds(pl.multiple_of(8 * (STEP * i + tile), 8), 8)
            swept[0, rows], swept[1, rows] = sweep_x(
                ext[rows, :128],
                ext[rows, 128:],
                scale * moved[rows, :128],
                scale * moved[rows, 128:],
            )
        return carry

    lax.fori_loop(0, EY * EZ // 8 // STEP, along_x, 0)
    for half in range(2):
        lanes = pl.ds(128 * half, 128)

        def along_y(tile, carry):
            held = [None] * EY
            for y in range(EY):
                rows = pl.ds(pl.multiple_of(8 * tile + EZ * y, 8), 8)
                parts = weights(swept[half, rows], scale * later[0, rows, lanes])
                for target in range(max(y - 6, 0), min(y + 1, FY)):
                    part = parts[target - y + 6]
                    held[target] = part if held[target] is None else held[target] + part
                if y >= 6:
                    slots = pl.ds(pl.multiple_of(8 * tile + EZ * (y - 6), 8), 8)
                    landed[half, slots] = held[y - 6]
            return carry

        lax.fori_loop(0, EZ // 8, along_y, 0)

    lane = lax.broadcasted_iota(jnp.int32, (8, 128), 1)
    pick = lax.div(lane, 2)
    is_odd = lax.rem(lane, 2) == 1

    def along_z(i, carry):
        for step in range(LINES):
            y = LINES * i + step
            here = pl.ds(pl.multiple_of(EZ * y, 8), EZ)
            there = pl.ds(pl.multiple_of(EZ * (y + 3), 8), EZ)
            totals = []
            for half in range(2):
                lanes = pl.ds(128 * half, 128)
                parts = weights(landed[half, here], scale * later[1, there, lanes])
                total = parts[3][:FZ]
                for k, offset in enumerate((-3, -2, -1, 1, 2, 3)):
                    part = parts[3 + offset]
                    room = shifts.at[step, half, k]
                    room[8:24, :] = part[:FZ]
                    if offset > 0:
                        room[0:8, :] = part[FZ:]
                    else:
                        room[24:32, :] = part[FZ:]
                    total = total + room[pl.ds(8 - offset, FZ), :]
                totals.append(total)
            for tile in range(FZ // 8):
                rows = slice(8 * tile, 8 * tile + 8)
                for half in range(2):
                    even, odd = (
                        jnp.take_along_axis(t[rows], pick + 64 * half, axis=1) for t in totals
                    )
                    out[y, rows, 128 * half : 128 * half + 128] = jnp.where(is_odd, odd, even)
        return carry

    lax.fori_loop(0, FY // LINES, along_z, 0)


def shards(vorticity, scalar):
    lines, block, parity = refine_tables()
    tables = [jnp.asarray(t) for t in spectral_tables() + (lines,)]
    tables += [jnp.asarray(block, jnp.bfloat16), jnp.asarray(parity, jnp.bfloat16)]
    vmem = pl.BlockSpec(memory_space=pltpu.VMEM)
    f32 = jnp.float32
    operands = [vorticity.reshape(3, YB * ZB, N), scalar] + tables
    moved, wide, ext, peak = pl.pallas_call(
        spectral_kernel,
        out_shape=(
            pltpu.VMEM((EY * EZ, 256), f32),
            pltpu.VMEM((4, 256, 256), jnp.bfloat16),
            pltpu.VMEM((EY, EZ, 256), f32),
            pltpu.VMEM((8, 128), f32),
        ),
        in_specs=[pl.BlockSpec(memory_space=pltpu.HBM)] * len(operands),
        out_specs=(vmem,) * 4,
        scratch_shapes=[
            pltpu.VMEM((3, 128, 128), f32),
            pltpu.VMEM((FY, FZ, 256), f32),
            *[pltpu.VMEM(t.shape, t.dtype) for t in tables],
            pltpu.VMEM((3, 2, 64, 128), f32),
            pltpu.VMEM((3, 2, 64, 128), f32),
            pltpu.VMEM((3, 128, 128), f32),
            pltpu.VMEM((3, 128, 128), f32),
            pltpu.VMEM((3, 128, 128), f32),
            pltpu.VMEM((3, 128, 128), f32),
            pltpu.VMEM((3, 2, 64, 128), f32),
            pltpu.VMEM((3, 2, 64, 128), f32),
            pltpu.VMEM((3, 256, 128), f32),
            pltpu.VMEM((3, 96, 128), f32),
            pltpu.VMEM((128, 128), f32),
            pltpu.SemaphoreType.DMA((13,)),
            pltpu.SemaphoreType.DMA((3,)),
            pltpu.SemaphoreType.DMA((3,)),
            pltpu.SemaphoreType.DMA((2, 3)),
            pltpu.SemaphoreType.DMA((2, 3)),
            pltpu.SemaphoreType.DMA((8,)),
            pltpu.SemaphoreType.DMA((8,)),
            pltpu.SemaphoreType.DMA((8,)),
            pltpu.SemaphoreType.DMA((8,)),
        ],
        compiler_params=pltpu.CompilerParams(
            collective_id=0, has_side_effects=True, vmem_limit_bytes=VMEM_LIMIT
        ),
        name="spectral",
    )(*[pltpu.with_memory_space_constraint(a, pltpu.HBM) for a in operands])
    return pl.pallas_call(
        remesh_kernel,
        out_shape=jax.ShapeDtypeStruct((FY, FZ, 256), f32),
        in_specs=[vmem] * 5,
        out_specs=vmem,
        scratch_shapes=[
            pltpu.VMEM((2, EY * EZ, 256), f32),
            pltpu.VMEM((2, EY * EZ, 128), f32),
            pltpu.VMEM((2, FY * EZ, 128), f32),
            pltpu.VMEM((LINES, 2, 6, 32, 128), f32),
        ],
        compiler_params=pltpu.CompilerParams(vmem_limit_bytes=VMEM_LIMIT),
        name="remesh",
    )(moved, wide, ext.reshape(EY * EZ, 256), peak, tables[-2])


def solution(mesh):
    return jax.shard_map(
        shards,
        mesh=mesh,
        in_specs=(P(None, "row", "col", None), P("row", "col", None)),
        out_specs=P("row", "col", None),
        check_vma=False,
    )
```
